32 devices in a mesh: tm: 16 (over z, x, core), freq: 2 (over y).
Axes of the slice: x: 2, y: 2, z: 4, core: 2. Of those that a mesh axis runs over, the one named last changes fastest.
Arguments:
- strengths: bfloat16 [2, 8, 256, 32768], P(None, 'freq', None, 'tm'), may hold values from -6 to 6
- sample_cell: int32 [32768], P('tm'), may hold values from 0 to 16383, as said below
- sample_frac: float32 [32768], P('tm'), may hold values from 0 to 1
Outputs:
- spectra: float32 [2, 8, 256, 4, 32, 128], P(None, None, 'tm', 'freq')
The draws below stay inside these ranges and needn't reach their ends.
Inputs may be any that keep to these rules, and one draw needn't show every extreme that they name: `sample_cell`: the samples of the i-th aligned block of 2048 samples lie in cells i * 1024 to (i + 1) * 1024 - 1; in every block the first sample lies in the first of these cells and the second sample in the last.
All inputs are finite; a program needn't handle non-finite values.
Results may differ from the reference program's by a relative error of at most 0.0037.
Values may be sent and summed in bfloat16 or wider, within the bound.
A program may use at most 128 MiB of HBM per device.

```python
import math
import jax
import jax.numpy as jnp
from jax import lax

TAPS = 8
FGROUPS = 8
CHG = 256
GRID_DEV = 1024
SAMP_DEV = 2048
FFT_LO = 32
FFT_HI = 128
FFTLEN = 4096
SAMPLES = 32768
CELLS = 16384
FRAMES = 4


def draw_sample_cell(key, part):
    offsets = jax.random.randint(key, (SAMPLES,), 0, GRID_DEV)
    within = jnp.arange(SAMPLES) % SAMP_DEV
    offsets = jnp.where(within == 0, 0, jnp.where(within == 1, GRID_DEV - 1, offsets))
    blocks = jnp.arange(SAMPLES) // SAMP_DEV
    return (blocks * GRID_DEV + offsets).astype(jnp.int32)


def levels(rng, dims, cuts, least, largest):
    gain, own = 1.0, jax.random.fold_in(rng, 6)
    for dim, blocks in cuts:
        heights = jnp.exp(jax.random.uniform(jax.random.fold_in(own, dim), (blocks,), jnp.float32, least / len(cuts), largest / len(cuts)))
        gain = gain * jnp.repeat(heights, dims[dim] // blocks).reshape([-1 if axis == dim else 1 for axis in range(len(dims))])
    return gain


def scatter_about(key, dims, scale, reach, shards=(), dtype=jnp.bfloat16):
    factor_of = levels(key, dims, shards, -0.22, 0.18) if shards else 1.0
    drawn = jax.random.normal(key, dims, jnp.float32) * scale * factor_of
    return jnp.minimum(jnp.maximum(drawn, -reach), reach).astype(dtype)


def setup_inputs(seed: int = 0) -> dict:
    splits = jax.random.split(jax.random.key(seed), 4)
    return {
        "strengths": scatter_about(splits[0], (2, FGROUPS, CHG, SAMPLES), 1.0, 6.0, ((1, 2), (3, 16))),
        "sample_cell": draw_sample_cell(jax.random.fold_in(splits[3], 71), 0),
        "sample_frac": jnp.clip(1.0 * jax.random.uniform(splits[2], (SAMPLES,), jnp.float32) ** levels(splits[2], (SAMPLES,), ((0, 16),), -0.2, 0.2), 0.0, 1.0),
    }


sharpness = 0.3

def one_group(group_strengths, sample_cell, sample_frac):
    values = group_strengths.astype(jnp.float32)
    accumulated = jnp.zeros((2, CHG, CELLS), jnp.float32)
    for tap_index in range(TAPS):
        shifted = jnp.float32(tap_index) - float(TAPS // 2 - 1) - sample_frac
        weight_row = lax.optimization_barrier(jnp.exp(-sharpness * (shifted * shifted)).astype(jnp.bfloat16)).astype(jnp.float32)
        target = ((sample_cell + (tap_index - (TAPS // 2 - 1))) % CELLS).astype(jnp.int32)
        accumulated = accumulated.at[:, :, target].add(values * weight_row)
    rounded = lax.optimization_barrier(accumulated.astype(jnp.bfloat16)).astype(jnp.float32)
    framed = rounded.reshape(2, CHG, FRAMES, FFTLEN)
    transform = jnp.fft.fft(framed[0] + 1j * framed[1], axis=-1) * (1.0 / math.sqrt(FFTLEN))
    parts = jnp.stack([jnp.real(transform), jnp.imag(transform)]).astype(jnp.float32)
    digits = parts.reshape(2, CHG, FRAMES, FFT_HI, FFT_LO)
    return jnp.swapaxes(digits, -1, -2)

def reference(strengths, sample_cell, sample_frac):
    by_group = jnp.moveaxis(strengths, 1, 0)
    result = lax.map(lambda group_strengths: one_group(group_strengths, sample_cell, sample_frac), by_group)
    return jnp.moveaxis(result, 0, 1)
```

```python
import functools
import math

import jax
import jax.numpy as jnp
import numpy as np
from jax import lax
from jax.experimental import pallas as pl
from jax.experimental.pallas import tpu as pltpu
from jax.sharding import PartitionSpec as P

TAPS = 8
HALF = TAPS // 2
GRID_DEV = 1024
FFT_LO = 32
FFT_HI = 128
FFTLEN = 4096
SHARP = 0.3
MESH = pl.DeviceIdType.MESH
LANES = 128
SLABS = GRID_DEV // LANES
INNER = SLABS - 2
PER_FRAME = FFTLEN // GRID_DEV
EARLY = 3
PLACE = [INNER] + list(range(INNER)) + [INNER + 1]


def fft_list(re, im):
    n = len(re)
    if n == 1:
        return re, im
    er, ei = fft_list(re[0::2], im[0::2])
    orr, oi = fft_list(re[1::2], im[1::2])
    out_r, out_i = [None] * n, [None] * n
    for k in range(n // 2):
        c, s = math.cos(2 * math.pi * k / n), math.sin(2 * math.pi * k / n)
        a, b = orr[k], oi[k]
        if k == 0:
            tr, ti = a, b
        elif 4 * k == n:
            tr, ti = b, -a
        elif 8 * k == n:
            tr, ti = (a + b) * c, (b - a) * c
        elif 8 * k == 3 * n:
            tr, ti = (b - a) * s, -(a + b) * s
        else:
            tr, ti = a * c + b * s, b * c - a * s
        out_r[k], out_i[k] = er[k] + tr, ei[k] + ti
        out_r[k + n // 2], out_i[k + n // 2] = er[k] - tr, ei[k] - ti
    return out_r, out_i


def spread_order(count):
    bits = count.bit_length() - 1
    if 1 << bits != count:
        return list(range(count))
    return [int(format(i, "0%db" % bits)[::-1], 2) if bits else 0 for i in range(count)]


def main_kernel(
    n_tm, n_fq, strengths, cell, frac, tc, ts, hi, y,
    xv, cols, fracs, inner_table, edge_table, edge_acc, edge_out, halo, src, recv, lhs,
    load, send, arrive, halo_send, halo_arrive,
):
    t = lax.axis_index("tm")
    f = lax.axis_index("freq")
    groups = xv.shape[0]
    chunk, samples = xv.shape[3], xv.shape[4]
    rows = src.shape[3]
    span = n_tm // n_fq
    frames = span // PER_FRAME
    slot = lax.rem(t, span)
    home = lax.div(t, span)
    half = n_tm // 2
    block = half * rows
    upper = lax.div(t, half)
    quarter = lax.div(t, n_tm // 4)
    outer = (quarter == 0) | (quarter == 3)
    right = lax.rem(t + 1, n_tm)
    left = lax.rem(t + n_tm - 1, n_tm)
    steps = 2 * groups
    early = min(EARLY, steps)
    keep = home == f

    def order(k):
        far = jnp.where(outer, lax.div(k, groups), 1 - lax.rem(k, 2))
        side = jnp.where(far == 1, 1 - upper, upper)
        return side, jnp.where(outer, lax.rem(k, groups), lax.div(k, 2))

    def fetch(g, d):
        channels = pl.ds(pl.multiple_of(d * chunk, chunk), chunk)
        return pltpu.make_async_copy(strengths.at[:, g, channels, :], xv.at[g, d], load.at[g, d])

    def fetch_step(k, c):
        side, g = order(k)

        def one(i, c):
            fetch(g, side * half + i).start()
            return c

        return lax.fori_loop(0, half, one, c)

    lax.fori_loop(0, steps, fetch_step, 0)

    def loaded(k):
        side, g = order(k)

        def one(i, c):
            fetch(g, side * half + i).wait()
            return c

        lax.fori_loop(0, half, one, 0)

    barrier = pltpu.get_barrier_semaphore()

    def greet(i, c):
        origin = f * span + lax.rem(slot + 1 + i, span)

        def one(j, c):
            other = lax.rem(f + j, n_fq)

            @pl.when((origin != t) | (other != f))
            def _():
                pl.semaphore_signal(barrier, inc=1, device_id=(origin, other), device_id_type=MESH)

            return c

        return lax.fori_loop(0, n_fq, one, c)

    lax.fori_loop(0, span, greet, 0)
    for peer in (left, right):
        pl.semaphore_signal(barrier, inc=1, device_id=(peer, f), device_id_type=MESH)

    base = t * GRID_DEV
    for i in range(samples // LANES):
        at = pl.ds(i * LANES, LANES)
        local = (cell[i : i + 1, :] - base).astype(jnp.float32)
        cols[at, :] = jnp.broadcast_to(local, (LANES, LANES)).T
        fracs[at, :] = jnp.broadcast_to(frac[i : i + 1, :], (LANES, LANES)).T
    lane = lax.broadcasted_iota(jnp.int32, (LANES, LANES), 1)

    def build(table, place, columns):
        def part(i, c):
            at = pl.ds(pl.multiple_of(i * LANES, LANES), LANES)
            d = columns - cols[at, :]
            u = d - fracs[at, :]
            w = jnp.exp(-SHARP * (u * u))
            inside = jnp.abs(d - 0.5) < float(HALF)
            table[at, place * LANES : (place + 1) * LANES] = jnp.where(inside, w, 0.0).astype(jnp.bfloat16)
            return c

        lax.fori_loop(0, samples // LANES, part, 0)

    def slab_columns(j):
        return (lane + j * LANES).astype(jnp.float32)

    def operand(k):
        side, g = order(k)
        return xv[g, pl.ds(side * half, half)].reshape(block, samples)

    def grid_inner(k, first, count):
        side, g = order(k)
        acc = jnp.dot(
            operand(k),
            inner_table[:, first * LANES : (first + count) * LANES],
            preferred_element_type=jnp.float32,
        ).astype(jnp.bfloat16)
        for i in range(half):
            for j in range(count):
                src[side * half + i, g, first + j] = acc[
                    i * rows : (i + 1) * rows, j * LANES : (j + 1) * LANES
                ]

    def copy_out(d, g, first, count):
        part = pl.ds(first, count)
        return pltpu.make_async_remote_copy(
            src_ref=src.at[d, g, part],
            dst_ref=recv.at[f, slot, g, part],
            send_sem=send.at[d, g],
            recv_sem=arrive.at[f, slot, g],
            device_id=(d, home),
            device_id_type=MESH,
        )

    spread = spread_order(half)

    def send_step(k, first, count):
        side, g = order(k)
        for i in range(half):
            d = side * half + lax.rem(t + spread[i], half)

            @pl.when((d != t) | (home != f))
            def _():
                copy_out(d, g, first, count).start()

    loaded(0)
    for b in range(INNER // 2):
        for j in range(2):
            build(inner_table, 2 * b + j, slab_columns(1 + 2 * b + j))
        grid_inner(0, 2 * b, 2)
        if b == 0:
            pl.semaphore_wait(barrier, jnp.where(keep, n_tm + 1, n_tm + 2))
        send_step(0, 2 * b, 2)

    beyond = jnp.where(
        lane < HALF, lane + GRID_DEV, jnp.where((lane >= 16 - HALF) & (lane < 16), lane - 16, -GRID_DEV)
    ).astype(jnp.float32)
    build(edge_table, 0, slab_columns(0))
    build(edge_table, 1, slab_columns(SLABS - 1))
    build(edge_table, 2, beyond)

    def row_block(k):
        side, g = order(k)
        return pl.ds(pl.multiple_of((g * 2 + side) * block, LANES), block)

    def edges(k, c):
        @pl.when(k > 0)
        def _():
            loaded(k)

        at = row_block(k)
        acc = jnp.dot(operand(k), edge_table[...], preferred_element_type=jnp.float32)
        edge_acc[at, :] = acc[:, : 2 * LANES]
        edge_out[:, at] = acc[:, 2 * LANES :].T[:16]
        return c

    lax.fori_loop(0, steps, edges, 0)
    halo[8 : LANES - 8, :] = jnp.zeros((LANES - 16, halo.shape[1]), jnp.float32)

    def halo_copy(i, peer):
        return pltpu.make_async_remote_copy(
            src_ref=edge_out.at[8 * i : 8 * i + 8],
            dst_ref=halo.at[pl.ds(i * (LANES - 8), 8)],
            send_sem=halo_send.at[i],
            recv_sem=halo_arrive.at[i],
            device_id=(peer, f),
            device_id_type=MESH,
        )

    halo_copy(0, right).start()
    halo_copy(1, left).start()

    def early_step(k, c):
        grid_inner(k, 0, INNER)
        send_step(k, 0, INNER)
        return c

    lax.fori_loop(1, early, early_step, 0)
    halo_copy(0, right).wait_recv()
    halo_copy(1, left).wait_recv()

    def finish_edges(k):
        side, g = order(k)
        at = row_block(k)
        acc = edge_acc[at, :]
        outside = halo[:, at].T
        spot = lax.broadcasted_iota(jnp.int32, (block, LANES), 1)
        low = acc[:, :LANES] + jnp.where(spot < LANES // 2, outside, 0.0)
        high = acc[:, LANES:] + jnp.where(spot >= LANES // 2, outside, 0.0)
        low, high = low.astype(jnp.bfloat16), high.astype(jnp.bfloat16)
        for i in range(half):
            src[side * half + i, g, INNER] = low[i * rows : (i + 1) * rows]
            src[side * half + i, g, INNER + 1] = high[i * rows : (i + 1) * rows]

    def early_edges(k, c):
        finish_edges(k)
        send_step(k, INNER, 2)
        return c

    lax.fori_loop(0, early, early_edges, 0)

    def late_step(k, c):
        grid_inner(k, 0, INNER)
        finish_edges(k)
        send_step(k, 0, SLABS)
        return c

    lax.fori_loop(early, steps, late_step, 0)

    @pl.when(keep)
    def _():
        def own(g, c):
            recv[f, slot, g] = src[t, g]
            return c

        lax.fori_loop(0, groups, own, 0)

    def landed(g, source, s):
        return pltpu.make_async_remote_copy(
            src_ref=src.at[0, g],
            dst_ref=recv.at[source, s, g],
            send_sem=send.at[0, g],
            recv_sem=arrive.at[source, s, g],
            device_id=(t, f),
            device_id_type=MESH,
        )

    flat = y.reshape(2, n_fq * groups, chunk * frames * FFT_LO, FFT_HI)

    def unit(i, c):
        turn = lax.div(i, groups * n_fq)
        m = lax.rem(turn + frames - 1 + f, frames)
        g = lax.rem(lax.div(i, n_fq), groups)
        source = lax.rem(f + lax.rem(i, n_fq), n_fq)

        def await_one(s, c):
            slot_in = m * PER_FRAME + s

            @pl.when((source != f) | (f * span + slot_in != t))
            def _():
                landed(g, source, slot_in).wait_recv()

            return c

        lax.fori_loop(0, PER_FRAME, await_one, 0)
        re, im = [], []
        for n in range(FFT_LO):
            tile = recv.at[source, m * PER_FRAME + n // SLABS, g, PLACE[n % SLABS]]
            re.append(tile[:chunk].astype(jnp.float32))
            im.append(tile[chunk:].astype(jnp.float32))
        re, im = fft_list(re, im)
        for a in range(FFT_LO):
            cc = tc[a : a + 1, :]
            ss = ts[a : a + 1, :]
            at = pl.ds(a * chunk, chunk)
            lhs[at, :FFT_HI] = (re[a] * cc + im[a] * ss).astype(jnp.bfloat16)
            lhs[at, FFT_HI:] = (im[a] * cc - re[a] * ss).astype(jnp.bfloat16)
        out = jnp.dot(lhs[...], hi[...], preferred_element_type=jnp.float32)
        for a in range(FFT_LO):
            for p in range(2):
                flat[p, source * groups + g, pl.ds(m * FFT_LO + a, chunk, stride=frames * FFT_LO), :] = out[
                    a * chunk : (a + 1) * chunk, p * FFT_HI : (p + 1) * FFT_HI
                ]
        return c

    lax.fori_loop(0, frames * groups * n_fq, unit, 0)

    def sent(i, c):
        d, g = lax.div(i, groups), lax.rem(i, groups)

        @pl.when((d != t) | (home != f))
        def _():
            copy_out(d, g, 0, SLABS).wait_send()

        return c

    lax.fori_loop(0, n_tm * groups, sent, 0)
    halo_copy(0, right).wait_send()
    halo_copy(1, left).wait_send()


def write_kernel(y, out, sems):
    parts, blocks = y.shape[0], y.shape[1]

    def copies():
        return [
            pltpu.make_async_copy(y.at[p, b], out.at[p, b], sems.at[p * blocks + b])
            for p in range(parts)
            for b in range(blocks)
        ]

    for c in copies():
        c.start()
    for c in copies():
        c.wait()


def shards(strengths, sample_cell, sample_frac):
    n_tm, n_fq = lax.axis_size("tm"), lax.axis_size("freq")
    parts, groups, channels, samples = strengths.shape
    span = n_tm // n_fq
    frames = span // PER_FRAME
    chunk = channels // n_tm
    rows = parts * chunk
    total = groups * n_tm * rows
    low = np.arange(FFT_LO)[:, None] * np.arange(FFT_HI)[None, :] * (2 * math.pi / FFTLEN)
    high = np.arange(FFT_HI)[:, None] * np.arange(FFT_HI)[None, :] % FFT_HI * (2 * math.pi / FFT_HI)
    hc, hs = np.cos(high), np.sin(high)
    full = np.block([[hc, -hs], [hs, hc]]).astype(np.float32) / math.sqrt(FFTLEN)
    vmem = pl.BlockSpec(memory_space=pltpu.VMEM)
    y_shape = (parts, n_fq * groups, chunk, frames, FFT_LO, FFT_HI)
    y = pl.pallas_call(
        functools.partial(main_kernel, n_tm, n_fq),
        out_shape=jax.ShapeDtypeStruct(y_shape, jnp.float32),
        in_specs=[pl.BlockSpec(memory_space=pl.ANY)] + [vmem] * 5,
        out_specs=vmem,
        scratch_shapes=[
            pltpu.VMEM((groups, n_tm, parts, chunk, samples), jnp.bfloat16),
            pltpu.VMEM((samples, LANES), jnp.float32),
            pltpu.VMEM((samples, LANES), jnp.float32),
            pltpu.VMEM((samples, INNER * LANES), jnp.bfloat16),
            pltpu.VMEM((samples, 3 * LANES), jnp.bfloat16),
            pltpu.VMEM((total, 2 * LANES), jnp.float32),
            pltpu.VMEM((16, total), jnp.float32),
            pltpu.VMEM((LANES, total), jnp.float32),
            pltpu.VMEM((n_tm, groups, SLABS, rows, LANES), jnp.bfloat16),
            pltpu.VMEM((n_fq, span, groups, SLABS, rows, LANES), jnp.bfloat16),
            pltpu.VMEM((FFT_LO * chunk, 2 * FFT_HI), jnp.bfloat16),
            pltpu.SemaphoreType.DMA((groups, n_tm)),
            pltpu.SemaphoreType.DMA((n_tm, groups)),
            pltpu.SemaphoreType.DMA((n_fq, span, groups)),
            pltpu.SemaphoreType.DMA((2,)),
            pltpu.SemaphoreType.DMA((2,)),
        ],
        compiler_params=pltpu.CompilerParams(
            collective_id=0, has_side_effects=True, vmem_limit_bytes=46 * 1024 * 1024
        ),
        name="grid_exchange_transform",
    )(
        strengths,
        sample_cell.reshape(samples // LANES, LANES),
        sample_frac.reshape(samples // LANES, LANES),
        jnp.asarray(np.cos(low), jnp.float32),
        jnp.asarray(np.sin(low), jnp.float32),
        jnp.asarray(full.astype(jnp.bfloat16)),
    )
    return pl.pallas_call(
        write_kernel,
        out_shape=jax.ShapeDtypeStruct(y_shape, jnp.float32),
        in_specs=[vmem],
        out_specs=pl.BlockSpec(memory_space=pl.ANY),
        scratch_shapes=[pltpu.SemaphoreType.DMA((parts * n_fq * groups,))],
        compiler_params=pltpu.CompilerParams(vmem_limit_bytes=16 * 1024 * 1024),
        name="write_out",
    )(y)


def solution(mesh):
    placed = (P(None, "freq", None, "tm"), P("tm"), P("tm"))
    return jax.shard_map(
        shards,
        mesh=mesh,
        in_specs=placed,
        out_specs=P(None, None, "tm", "freq", None, None),
        check_vma=False,
    )
```

```python
import functools
import math

import jax
import jax.numpy as jnp
import numpy as np
from jax import lax
from jax.experimental import pallas as pl
from jax.experimental.pallas import tpu as pltpu
from jax.sharding import PartitionSpec as P

TAPS = 8
HALF = TAPS // 2
GRID_DEV = 1024
FFT_LO = 32
FFT_HI = 128
FFTLEN = 4096
SHARP = 0.3
MESH = pl.DeviceIdType.MESH
LANES = 128
SLABS = GRID_DEV // LANES
INNER = SLABS - 2
PER_FRAME = FFTLEN // GRID_DEV
EARLY = 3
FIRST = ((0, 2), (2, 4))
PLACE = [INNER] + list(range(INNER)) + [INNER + 1]


def fft_list(re, im):
    n = len(re)
    if n == 1:
        return re, im
    er, ei = fft_list(re[0::2], im[0::2])
    orr, oi = fft_list(re[1::2], im[1::2])
    out_r, out_i = [None] * n, [None] * n
    for k in range(n // 2):
        c, s = math.cos(2 * math.pi * k / n), math.sin(2 * math.pi * k / n)
        a, b = orr[k], oi[k]
        if k == 0:
            tr, ti = a, b
        elif 4 * k == n:
            tr, ti = b, -a
        elif 8 * k == n:
            tr, ti = (a + b) * c, (b - a) * c
        elif 8 * k == 3 * n:
            tr, ti = (b - a) * s, -(a + b) * s
        else:
            tr, ti = a * c + b * s, b * c - a * s
        out_r[k], out_i[k] = er[k] + tr, ei[k] + ti
        out_r[k + n // 2], out_i[k + n // 2] = er[k] - tr, ei[k] - ti
    return out_r, out_i


def spread_order(count):
    bits = count.bit_length() - 1
    if 1 << bits != count:
        return list(range(count))
    return [int(format(i, "0%db" % bits)[::-1], 2) if bits else 0 for i in range(count)]


def main_kernel(
    n_tm, n_fq, strengths, cell_hbm, frac_hbm, tc_hbm, ts_hbm, hi_hbm, y,
    xv, cell, frac, tc, ts, hi, cols, fracs, table, edge_out, halo, src, recv, lhs,
    small, load, send, arrive, halo_send, halo_arrive,
):
    t = lax.axis_index("tm")
    f = lax.axis_index("freq")
    parts, groups, channels, samples = xv.shape
    chunk = channels // n_tm
    rows = src.shape[3]
    wide = channels // 2
    both = 2 if groups % 2 == 0 else 1
    span = n_tm // n_fq
    frames = span // PER_FRAME
    slot = lax.rem(t, span)
    home = lax.div(t, span)
    half = n_tm // 2
    block = half * rows
    upper = lax.div(t, half)
    quarter = lax.div(t, n_tm // 4)
    outer = (quarter == 0) | (quarter == 3)
    right = lax.rem(t + 1, n_tm)
    left = lax.rem(t + n_tm - 1, n_tm)
    steps = 2 * groups
    early = min(EARLY, steps)
    keep = home == f

    def order(k):
        ahead = (k == 0) | ((lax.rem(k, 2) == 1) & (k < steps - 1))
        far = jnp.where(outer, k >= groups, ahead)
        inward = jnp.where(ahead, lax.div(k + 1, 2), lax.div(k - 1, 2))
        side = jnp.where(far, 1 - upper, upper)
        return side, jnp.where(outer, lax.rem(k, groups), inward)

    constants = [
        pltpu.make_async_copy(a, b, small.at[i])
        for i, (a, b) in enumerate(
            ((cell_hbm, cell), (frac_hbm, frac), (tc_hbm, tc), (ts_hbm, ts), (hi_hbm, hi))
        )
    ]
    for i in range(2):
        constants[i].start()

    def fetch(k):
        side, g = order(k)
        at = (slice(None), g, pl.ds(pl.multiple_of(side * wide, wide), wide))
        return pltpu.make_async_copy(strengths.at[at], xv.at[at], load.at[k])

    fetch(0).start()

    barrier = pltpu.get_barrier_semaphore()

    def greet(i, c):
        origin = f * span + lax.rem(slot + 1 + i, span)

        def one(j, c):
            other = lax.rem(f + j, n_fq)

            @pl.when((origin != t) | (other != f))
            def _():
                pl.semaphore_signal(barrier, inc=1, device_id=(origin, other), device_id_type=MESH)

            return c

        return lax.fori_loop(0, n_fq, one, c)

    lax.fori_loop(0, span, greet, 0)
    for peer in (left, right):
        pl.semaphore_signal(barrier, inc=1, device_id=(peer, f), device_id_type=MESH)

    for k in range(1, steps):
        fetch(k).start()

    base = t * GRID_DEV
    constants[0].wait()
    constants[1].wait()
    for i in range(samples // LANES):
        at = pl.ds(i * LANES, LANES)
        local = (cell[i : i + 1, :] - base).astype(jnp.float32)
        cols[at, :] = jnp.broadcast_to(local, (LANES, LANES)).T
        fracs[at, :] = jnp.broadcast_to(frac[i : i + 1, :], (LANES, LANES)).T
    lane = lax.broadcasted_iota(jnp.int32, (LANES, LANES), 1)

    def build(place, columns):
        def part(i, c):
            at = pl.ds(pl.multiple_of(i * LANES, LANES), LANES)
            d = columns - cols[at, :]
            u = d - fracs[at, :]
            w = jnp.exp(-SHARP * (u * u))
            inside = jnp.abs(d - 0.5) < float(HALF)
            table[at, place * LANES : (place + 1) * LANES] = jnp.where(inside, w, 0.0).astype(jnp.bfloat16)
            return c

        lax.fori_loop(0, samples // LANES, part, 0, unroll=4)

    def slab_columns(j):
        return (lane + j * LANES).astype(jnp.float32)

    def operand(k):
        side, g = order(k)
        at = pl.ds(pl.multiple_of(side * wide, wide), wide)
        return xv[:, g, at, :].reshape(block, samples)

    def product(k, first, count):
        return jnp.dot(
            operand(k),
            table[:, first * LANES : (first + count) * LANES],
            preferred_element_type=jnp.float32,
        )

    def put(k, first, pieces):
        side, g = order(k)
        for j, part in enumerate(pieces):
            part = part.astype(jnp.bfloat16)
            for i in range(half):
                for p in range(parts):
                    start = p * wide + i * chunk
                    src[side * half + i, g, first + j, p * chunk : (p + 1) * chunk] = part[start : start + chunk]

    def slabs(acc):
        return [acc[:, j : j + LANES] for j in range(0, acc.shape[1], LANES)]

    def with_halo(k, low, high):
        side, g = order(k)
        outside = jnp.concatenate(
            [
                halo[:, pl.ds(pl.multiple_of(g * 2 * block + p * channels + side * wide, LANES), wide)].T
                for p in range(parts)
            ]
        )
        spot = lax.broadcasted_iota(jnp.int32, (block, LANES), 1)
        return [
            low + jnp.where(spot < LANES // 2, outside, 0.0),
            high + jnp.where(spot >= LANES // 2, outside, 0.0),
        ]

    def copy_out(d, g, first, count, pair=1):
        part = (pl.ds(g, pair), pl.ds(first, count))
        return pltpu.make_async_remote_copy(
            src_ref=src.at[(d,) + part],
            dst_ref=recv.at[(f, slot) + part],
            send_sem=send.at[d, g],
            recv_sem=arrive.at[f, slot, g],
            device_id=(d, home),
            device_id_type=MESH,
        )

    spread = spread_order(half)

    def send_step(k, first, count, pair=1):
        side, g = order(k)
        for i in range(half):
            d = side * half + lax.rem(t + spread[i], half)

            @pl.when((d != t) | (home != f))
            def _():
                copy_out(d, g - (pair - 1), first, count, pair).start()

    fetch(0).wait()
    with jax.named_scope("first"):
        for first, count in FIRST:
            for j in range(first, first + count):
                build(j, slab_columns(1 + j))
            put(0, first, slabs(product(0, first, count)))
            if first == 0:
                pl.semaphore_wait(barrier, jnp.where(keep, n_tm + 1, n_tm + 2))
            send_step(0, first, count)
            if first == 0:
                for i in range(2, 5):
                    constants[i].start()

    beyond = jnp.where(
        lane < HALF, lane + GRID_DEV, jnp.where((lane >= 16 - HALF) & (lane < 16), lane - 16, -GRID_DEV)
    ).astype(jnp.float32)

    def edges(g, c):
        acc = jnp.dot(
            xv[:, g].reshape(2 * block, samples),
            table[:, SLABS * LANES :],
            preferred_element_type=jnp.float32,
        )
        edge_out[:, pl.ds(pl.multiple_of(g * 2 * block, LANES), 2 * block)] = acc.T[:16]
        return c

    with jax.named_scope("edges"):
        build(SLABS, beyond)
        for k in range(1, steps):
            fetch(k).wait()
        lax.fori_loop(0, groups, edges, 0)
        halo[8 : LANES - 8, :] = jnp.zeros((LANES - 16, halo.shape[1]), jnp.float32)

    def halo_copy(i, peer):
        return pltpu.make_async_remote_copy(
            src_ref=edge_out.at[8 * i : 8 * i + 8],
            dst_ref=halo.at[pl.ds(i * (LANES - 8), 8)],
            send_sem=halo_send.at[i],
            recv_sem=halo_arrive.at[i],
            device_id=(peer, f),
            device_id_type=MESH,
        )

    halo_copy(0, right).start()
    halo_copy(1, left).start()

    def early_step(k, c):
        put(k, 0, slabs(product(k, 0, INNER)))
        send_step(k, 0, INNER)
        return c

    with jax.named_scope("early"):
        lax.fori_loop(1, early, early_step, 0)
        build(INNER, slab_columns(0))
        build(INNER + 1, slab_columns(SLABS - 1))
    with jax.named_scope("halo_wait"):
        halo_copy(0, right).wait_recv()
        halo_copy(1, left).wait_recv()

    def early_edges(k, c):
        put(k, INNER, with_halo(k, *slabs(product(k, INNER, 2))))
        send_step(k, INNER, 2)
        return c

    def late_step(k, c):
        pieces = slabs(product(k, 0, SLABS))
        put(k, 0, pieces[:INNER] + with_halo(k, *pieces[INNER:]))
        if both == 1:
            send_step(k, 0, SLABS)
        else:
            in_pairs = outer & (k >= groups)

            @pl.when(in_pairs & (lax.rem(k, 2) == 1))
            def _():
                send_step(k, 0, SLABS, both)

            @pl.when(jnp.logical_not(in_pairs))
            def _():
                send_step(k, 0, SLABS)

        return c

    with jax.named_scope("early_edges"):
        lax.fori_loop(0, early, early_edges, 0)
    with jax.named_scope("late"):
        lax.fori_loop(early, steps, late_step, 0)

    @pl.when(keep)
    def _():
        def own(g, c):
            recv[f, slot, g] = src[t, g]
            return c

        lax.fori_loop(0, groups, own, 0)

    def landed(source, s, g, pair=1):
        return pltpu.make_async_remote_copy(
            src_ref=src.at[0, pl.ds(g, pair)],
            dst_ref=recv.at[source, s, pl.ds(g, pair)],
            send_sem=send.at[0, g],
            recv_sem=arrive.at[source, s, g],
            device_id=(t, f),
            device_id_type=MESH,
        )

    def is_outer(index):
        q = lax.div(index, n_tm // 4)
        return (q == 0) | (q == 3)

    def paired(origin, d):
        return is_outer(origin) & (lax.div(origin, half) != lax.div(d, half)) & (both == 2)

    for i in range(2, 5):
        constants[i].wait()
    flat = y.reshape(2, n_fq * groups, chunk * frames * FFT_LO, FFT_HI)
    ready = min(2, groups)
    turns = frames * groups

    def sent(i, c):
        d, g = lax.div(i, groups), lax.rem(i, groups)
        away = (d != t) | (home != f)
        two = paired(t, d)

        @pl.when(away & jnp.logical_not(two))
        def _():
            copy_out(d, g, 0, SLABS).wait_send()

        if both == 2:

            @pl.when(away & two & (lax.rem(g, 2) == 0))
            def _():
                copy_out(d, g, 0, SLABS, both).wait_send()

        return c

    def unit(i, c):
        n = lax.div(i, n_fq)
        source = lax.rem(f + lax.rem(i, n_fq), n_fq)
        late = n - (turns - groups)
        first = n < ready
        last = (late >= ready) & (late >= 0)
        inward = first | last
        g = jnp.where(first, n, jnp.where(last, late, lax.rem(n - ready, groups)))
        m = jnp.where(inward, 0, 1 + lax.div(n - ready, groups))
        m = lax.rem(m + frames - 1 + f, frames)

        def await_one(s, c):
            slot_in = m * PER_FRAME + s
            origin = f * span + slot_in
            away = (source != f) | (origin != t)
            two = paired(origin, t)

            @pl.when(away & jnp.logical_not(two))
            def _():
                landed(source, slot_in, g).wait_recv()

            if both == 2:

                @pl.when(away & two & (lax.rem(g, 2) == 0))
                def _():
                    landed(source, slot_in, g, both).wait_recv()

            return c

        with jax.named_scope("await"):
            lax.fori_loop(0, PER_FRAME, await_one, 0)
        re, im = [], []
        for n in range(FFT_LO):
            tile = recv.at[source, m * PER_FRAME + n // SLABS, g, PLACE[n % SLABS]]
            re.append(tile[:chunk].astype(jnp.float32))
            im.append(tile[chunk:].astype(jnp.float32))
        re, im = fft_list(re, im)
        for a in range(FFT_LO):
            cc = tc[a : a + 1, :]
            ss = ts[a : a + 1, :]
            at = pl.ds(a * chunk, chunk)
            lhs[at, :FFT_HI] = (re[a] * cc + im[a] * ss).astype(jnp.bfloat16)
            lhs[at, FFT_HI:] = (im[a] * cc - re[a] * ss).astype(jnp.bfloat16)
        out = jnp.dot(lhs[...], hi[...], preferred_element_type=jnp.float32)
        for a in range(FFT_LO):
            for p in range(2):
                flat[p, source * groups + g, pl.ds(m * FFT_LO + a, chunk, stride=frames * FFT_LO), :] = out[
                    a * chunk : (a + 1) * chunk, p * FFT_HI : (p + 1) * FFT_HI
                ]
        return c

    lax.fori_loop(0, turns * n_fq, unit, 0)
    with jax.named_scope("sent"):
        lax.fori_loop(0, n_tm * groups, sent, 0)
        halo_copy(0, right).wait_send()
        halo_copy(1, left).wait_send()


def write_kernel(y, out, sems):
    parts, blocks = y.shape[0], y.shape[1]

    def copies():
        return [
            pltpu.make_async_copy(y.at[p, b], out.at[p, b], sems.at[p * blocks + b])
            for p in range(parts)
            for b in range(blocks)
        ]

    for c in copies():
        c.start()
    for c in copies():
        c.wait()


def shards(strengths, sample_cell, sample_frac):
    n_tm, n_fq = lax.axis_size("tm"), lax.axis_size("freq")
    parts, groups, channels, samples = strengths.shape
    span = n_tm // n_fq
    frames = span // PER_FRAME
    chunk = channels // n_tm
    rows = parts * chunk
    total = groups * n_tm * rows
    low = np.arange(FFT_LO)[:, None] * np.arange(FFT_HI)[None, :] * (2 * math.pi / FFTLEN)
    high = np.arange(FFT_HI)[:, None] * np.arange(FFT_HI)[None, :] % FFT_HI * (2 * math.pi / FFT_HI)
    hc, hs = np.cos(high), np.sin(high)
    full = np.block([[hc, -hs], [hs, hc]]).astype(np.float32) / math.sqrt(FFTLEN)
    vmem = pl.BlockSpec(memory_space=pltpu.VMEM)
    y_shape = (parts, n_fq * groups, chunk, frames, FFT_LO, FFT_HI)
    y = pl.pallas_call(
        functools.partial(main_kernel, n_tm, n_fq),
        out_shape=pltpu.VMEM(y_shape, jnp.float32),
        in_specs=[pl.BlockSpec(memory_space=pltpu.HBM)] * 6,
        out_specs=vmem,
        scratch_shapes=[
            pltpu.VMEM((parts, groups, channels, samples), jnp.bfloat16),
            pltpu.VMEM((samples // LANES, LANES), jnp.int32),
            pltpu.VMEM((samples // LANES, LANES), jnp.float32),
            pltpu.VMEM((FFT_LO, FFT_HI), jnp.float32),
            pltpu.VMEM((FFT_LO, FFT_HI), jnp.float32),
            pltpu.VMEM((2 * FFT_HI, 2 * FFT_HI), jnp.bfloat16),
            pltpu.VMEM((samples, LANES), jnp.float32),
            pltpu.VMEM((samples, LANES), jnp.float32),
            pltpu.VMEM((samples, (SLABS + 1) * LANES), jnp.bfloat16),
            pltpu.VMEM((16, total), jnp.float32),
            pltpu.VMEM((LANES, total), jnp.float32),
            pltpu.VMEM((n_tm, groups, SLABS, rows, LANES), jnp.bfloat16),
            pltpu.VMEM((n_fq, span, groups, SLABS, rows, LANES), jnp.bfloat16),
            pltpu.VMEM((FFT_LO * chunk, 2 * FFT_HI), jnp.bfloat16),
            pltpu.SemaphoreType.DMA((5,)),
            pltpu.SemaphoreType.DMA((2 * groups,)),
            pltpu.SemaphoreType.DMA((n_tm, groups)),
            pltpu.SemaphoreType.DMA((n_fq, span, groups)),
            pltpu.SemaphoreType.DMA((2,)),
            pltpu.SemaphoreType.DMA((2,)),
        ],
        compiler_params=pltpu.CompilerParams(
            collective_id=0, has_side_effects=True, vmem_limit_bytes=54 * 1024 * 1024
        ),
        name="grid_exchange_transform",
    )(
        strengths,
        sample_cell.reshape(samples // LANES, LANES),
        sample_frac.reshape(samples // LANES, LANES),
        jnp.asarray(np.cos(low), jnp.float32),
        jnp.asarray(np.sin(low), jnp.float32),
        jnp.asarray(full.astype(jnp.bfloat16)),
    )
    return pl.pallas_call(
        write_kernel,
        out_shape=jax.ShapeDtypeStruct(y_shape, jnp.float32),
        in_specs=[vmem],
        out_specs=pl.BlockSpec(memory_space=pl.ANY),
        scratch_shapes=[pltpu.SemaphoreType.DMA((parts * n_fq * groups,))],
        compiler_params=pltpu.CompilerParams(vmem_limit_bytes=16 * 1024 * 1024),
        name="write_out",
    )(y)


def solution(mesh):
    placed = (P(None, "freq", None, "tm"), P("tm"), P("tm"))
    return jax.shard_map(
        shards,
        mesh=mesh,
        in_specs=placed,
        out_specs=P(None, None, "tm", "freq", None, None),
        check_vma=False,
    )
```

```python
import functools
import math

import jax
import jax.numpy as jnp
import numpy as np
from jax import lax
from jax.experimental import pallas as pl
from jax.experimental.pallas import tpu as pltpu
from jax.sharding import PartitionSpec as P

TAPS = 8
HALF = TAPS // 2
GRID_DEV = 1024
FFT_LO = 32
FFT_HI = 128
FFTLEN = 4096
SHARP = 0.3
MESH = pl.DeviceIdType.MESH
LANES = 128
SLABS = GRID_DEV // LANES
INNER = SLABS - 2
PER_FRAME = FFTLEN // GRID_DEV
EARLY = 3
FIRST = ((0, 2), (2, 4))
PLACE = [INNER] + list(range(INNER)) + [INNER + 1]


def fft_list(re, im):
    n = len(re)
    if n == 1:
        return re, im
    er, ei = fft_list(re[0::2], im[0::2])
    orr, oi = fft_list(re[1::2], im[1::2])
    out_r, out_i = [None] * n, [None] * n
    for k in range(n // 2):
        c, s = math.cos(2 * math.pi * k / n), math.sin(2 * math.pi * k / n)
        a, b = orr[k], oi[k]
        if k == 0:
            tr, ti = a, b
        elif 4 * k == n:
            tr, ti = b, -a
        elif 8 * k == n:
            tr, ti = (a + b) * c, (b - a) * c
        elif 8 * k == 3 * n:
            tr, ti = (b - a) * s, -(a + b) * s
        else:
            tr, ti = a * c + b * s, b * c - a * s
        out_r[k], out_i[k] = er[k] + tr, ei[k] + ti
        out_r[k + n // 2], out_i[k + n // 2] = er[k] - tr, ei[k] - ti
    return out_r, out_i


def spread_order(count):
    bits = count.bit_length() - 1
    if 1 << bits != count:
        return list(range(count))
    return [int(format(i, "0%db" % bits)[::-1], 2) if bits else 0 for i in range(count)]


def transform(blocks, m, g, chunk, tc, ts, hi, lhs, out, start, stride):
    re, im = [], []
    for n in range(FFT_LO):
        tile = blocks[m * PER_FRAME + n // SLABS, g, PLACE[n % SLABS]]
        re.append(tile[:chunk].astype(jnp.float32))
        im.append(tile[chunk:].astype(jnp.float32))
    re, im = fft_list(re, im)
    for a in range(FFT_LO):
        cc = tc[a : a + 1, :]
        ss = ts[a : a + 1, :]
        at = pl.ds(a * chunk, chunk)
        lhs[at, :FFT_HI] = (re[a] * cc + im[a] * ss).astype(jnp.bfloat16)
        lhs[at, FFT_HI:] = (im[a] * cc - re[a] * ss).astype(jnp.bfloat16)
    y = jnp.dot(lhs[...], hi[...], preferred_element_type=jnp.float32)
    for a in range(FFT_LO):
        for p in range(2):
            out[p, pl.ds(start + a, chunk, stride=stride), :] = y[
                a * chunk : (a + 1) * chunk, p * FFT_HI : (p + 1) * FFT_HI
            ]


def main_kernel(
    n_tm, n_fq, strengths, cell_hbm, frac_hbm, tc_hbm, ts_hbm, hi_hbm, y, recv, tc, ts, hi,
    xv, cell, frac, cols, fracs, table, edge_out, halo, src, lhs,
    small, load, send, arrive, halo_send, halo_arrive,
):
    t = lax.axis_index("tm")
    f = lax.axis_index("freq")
    parts, groups, channels, samples = xv.shape
    chunk = channels // n_tm
    rows = src.shape[3]
    wide = channels // 2
    both = 2 if groups % 2 == 0 else 1
    span = n_tm // n_fq
    frames = span // PER_FRAME
    slot = lax.rem(t, span)
    home = lax.div(t, span)
    half = n_tm // 2
    block = half * rows
    upper = lax.div(t, half)
    quarter = lax.div(t, n_tm // 4)
    outer = (quarter == 0) | (quarter == 3)
    right = lax.rem(t + 1, n_tm)
    left = lax.rem(t + n_tm - 1, n_tm)
    steps = 2 * groups
    early = min(EARLY, steps)
    keep = home == f

    def order(k):
        ahead = (k == 0) | ((lax.rem(k, 2) == 1) & (k < steps - 1))
        far = jnp.where(outer, k >= groups, ahead)
        inward = jnp.where(ahead, lax.div(k + 1, 2), lax.div(k - 1, 2))
        side = jnp.where(far, 1 - upper, upper)
        return side, jnp.where(outer, lax.rem(k, groups), inward)

    constants = [
        pltpu.make_async_copy(a, b, small.at[i])
        for i, (a, b) in enumerate(
            ((cell_hbm, cell), (frac_hbm, frac), (tc_hbm, tc), (ts_hbm, ts), (hi_hbm, hi))
        )
    ]
    for i in range(2):
        constants[i].start()

    def fetch(k):
        side, g = order(k)
        at = (slice(None), g, pl.ds(pl.multiple_of(side * wide, wide), wide))
        return pltpu.make_async_copy(strengths.at[at], xv.at[at], load.at[k])

    fetch(0).start()

    barrier = pltpu.get_barrier_semaphore()

    def greet(i, c):
        origin = f * span + lax.rem(slot + 1 + i, span)

        def one(j, c):
            other = lax.rem(f + j, n_fq)

            @pl.when((origin != t) | (other != f))
            def _():
                pl.semaphore_signal(barrier, inc=1, device_id=(origin, other), device_id_type=MESH)

            return c

        return lax.fori_loop(0, n_fq, one, c)

    lax.fori_loop(0, span, greet, 0)
    for peer in (left, right):
        pl.semaphore_signal(barrier, inc=1, device_id=(peer, f), device_id_type=MESH)

    for k in range(1, steps):
        fetch(k).start()

    base = t * GRID_DEV
    constants[0].wait()
    constants[1].wait()
    for i in range(samples // LANES):
        at = pl.ds(i * LANES, LANES)
        local = (cell[i : i + 1, :] - base).astype(jnp.float32)
        cols[at, :] = jnp.broadcast_to(local, (LANES, LANES)).T
        fracs[at, :] = jnp.broadcast_to(frac[i : i + 1, :], (LANES, LANES)).T
    lane = lax.broadcasted_iota(jnp.int32, (LANES, LANES), 1)

    def build(place, columns):
        def part(i, c):
            at = pl.ds(pl.multiple_of(i * LANES, LANES), LANES)
            d = columns - cols[at, :]
            u = d - fracs[at, :]
            w = jnp.exp(-SHARP * (u * u))
            inside = jnp.abs(d - 0.5) < float(HALF)
            table[at, place * LANES : (place + 1) * LANES] = jnp.where(inside, w, 0.0).astype(jnp.bfloat16)
            return c

        lax.fori_loop(0, samples // LANES, part, 0, unroll=4)

    def slab_columns(j):
        return (lane + j * LANES).astype(jnp.float32)

    def operand(k):
        side, g = order(k)
        at = pl.ds(pl.multiple_of(side * wide, wide), wide)
        return xv[:, g, at, :].reshape(block, samples)

    def product(k, first, count):
        return jnp.dot(
            operand(k),
            table[:, first * LANES : (first + count) * LANES],
            preferred_element_type=jnp.float32,
        )

    def put(k, first, pieces):
        side, g = order(k)
        for j, part in enumerate(pieces):
            part = part.astype(jnp.bfloat16)
            for i in range(half):
                for p in range(parts):
                    start = p * wide + i * chunk
                    src[side * half + i, g, first + j, p * chunk : (p + 1) * chunk] = part[start : start + chunk]

    def slabs(acc):
        return [acc[:, j : j + LANES] for j in range(0, acc.shape[1], LANES)]

    def with_halo(k, low, high):
        side, g = order(k)
        outside = jnp.concatenate(
            [
                halo[:, pl.ds(pl.multiple_of(g * 2 * block + p * channels + side * wide, LANES), wide)].T
                for p in range(parts)
            ]
        )
        spot = lax.broadcasted_iota(jnp.int32, (block, LANES), 1)
        return [
            low + jnp.where(spot < LANES // 2, outside, 0.0),
            high + jnp.where(spot >= LANES // 2, outside, 0.0),
        ]

    def copy_out(d, g, first, count, pair=1):
        part = (pl.ds(g, pair), pl.ds(first, count))
        return pltpu.make_async_remote_copy(
            src_ref=src.at[(d,) + part],
            dst_ref=recv.at[(f, slot) + part],
            send_sem=send.at[lax.div(d, half), g],
            recv_sem=arrive.at[f, slot, g],
            device_id=(d, home),
            device_id_type=MESH,
        )

    spread = spread_order(half)

    def send_step(k, first, count, pair=1):
        side, g = order(k)
        for i in range(half):
            d = side * half + lax.rem(t + spread[i], half)

            @pl.when((d != t) | (home != f))
            def _():
                copy_out(d, g - (pair - 1), first, count, pair).start()

    fetch(0).wait()
    with jax.named_scope("first"):
        for first, count in FIRST:
            for j in range(first, first + count):
                build(j, slab_columns(1 + j))
            put(0, first, slabs(product(0, first, count)))
            if first == 0:
                pl.semaphore_wait(barrier, jnp.where(keep, n_tm + 1, n_tm + 2))
            send_step(0, first, count)
            if first == 0:
                for i in range(2, 5):
                    constants[i].start()

    beyond = jnp.where(
        lane < HALF, lane + GRID_DEV, jnp.where((lane >= 16 - HALF) & (lane < 16), lane - 16, -GRID_DEV)
    ).astype(jnp.float32)

    def edges(g, c):
        acc = jnp.dot(
            xv[:, g].reshape(2 * block, samples),
            table[:, SLABS * LANES :],
            preferred_element_type=jnp.float32,
        )
        edge_out[:, pl.ds(pl.multiple_of(g * 2 * block, LANES), 2 * block)] = acc.T[:16]
        return c

    with jax.named_scope("edges"):
        build(SLABS, beyond)
        for k in range(1, steps):
            fetch(k).wait()
        lax.fori_loop(0, groups, edges, 0)
        halo[8 : LANES - 8, :] = jnp.zeros((LANES - 16, halo.shape[1]), jnp.float32)

    def halo_copy(i, peer):
        return pltpu.make_async_remote_copy(
            src_ref=edge_out.at[8 * i : 8 * i + 8],
            dst_ref=halo.at[pl.ds(i * (LANES - 8), 8)],
            send_sem=halo_send.at[i],
            recv_sem=halo_arrive.at[i],
            device_id=(peer, f),
            device_id_type=MESH,
        )

    halo_copy(0, right).start()
    halo_copy(1, left).start()

    def early_step(k, c):
        put(k, 0, slabs(product(k, 0, INNER)))
        send_step(k, 0, INNER)
        return c

    with jax.named_scope("early"):
        lax.fori_loop(1, early, early_step, 0)
        build(INNER, slab_columns(0))
        build(INNER + 1, slab_columns(SLABS - 1))
    with jax.named_scope("halo_wait"):
        halo_copy(0, right).wait_recv()
        halo_copy(1, left).wait_recv()

    def early_edges(k, c):
        put(k, INNER, with_halo(k, *slabs(product(k, INNER, 2))))
        send_step(k, INNER, 2)
        return c

    def late_step(k, c):
        pieces = slabs(product(k, 0, SLABS))
        put(k, 0, pieces[:INNER] + with_halo(k, *pieces[INNER:]))
        if both == 1:
            send_step(k, 0, SLABS)
        else:
            in_pairs = outer & (k >= groups)

            @pl.when(in_pairs & (lax.rem(k, 2) == 1))
            def _():
                send_step(k, 0, SLABS, both)

            @pl.when(jnp.logical_not(in_pairs))
            def _():
                send_step(k, 0, SLABS)

        return c

    with jax.named_scope("early_edges"):
        lax.fori_loop(0, early, early_edges, 0)
    with jax.named_scope("late"):
        lax.fori_loop(early, steps, late_step, 0)

    @pl.when(keep)
    def _():
        def own(g, c):
            recv[f, slot, g] = src[t, g]
            return c

        lax.fori_loop(0, groups, own, 0)

    def landed(source, s, g, pair=1):
        return pltpu.make_async_remote_copy(
            src_ref=src.at[0, pl.ds(g, pair)],
            dst_ref=recv.at[source, s, pl.ds(g, pair)],
            send_sem=send.at[0, 0],
            recv_sem=arrive.at[source, s, g],
            device_id=(t, f),
            device_id_type=MESH,
        )

    def is_outer(index):
        q = lax.div(index, n_tm // 4)
        return (q == 0) | (q == 3)

    def paired(origin, d):
        return is_outer(origin) & (lax.div(origin, half) != lax.div(d, half)) & (both == 2)

    for i in range(2, 5):
        constants[i].wait()
    flat = y.reshape(2, n_fq * groups, chunk * frames * FFT_LO, FFT_HI)
    ready = min(2, groups)
    turns = frames * groups

    def sent(side, g, count, pair=1):
        part = src.at[pl.ds(side * half, count), pl.ds(g, pair)]
        pltpu.make_async_remote_copy(
            src_ref=part,
            dst_ref=part,
            send_sem=send.at[side, g],
            recv_sem=arrive.at[0, 0, 0],
            device_id=(right, f),
            device_id_type=MESH,
        ).wait_send()

    def all_sent(g, c):
        @pl.when(keep)
        def _():
            sent(upper, g, half - 1)

        @pl.when(jnp.logical_not(keep))
        def _():
            sent(upper, g, half)

        if both == 1:
            sent(1 - upper, g, half)
        else:

            @pl.when(jnp.logical_not(outer))
            def _():
                sent(1 - upper, g, half)

            @pl.when(outer & (lax.rem(g, 2) == 0))
            def _():
                sent(1 - upper, g, half, both)

        return c

    def await_unit(source, m, g):
        def await_one(s, c):
            slot_in = m * PER_FRAME + s
            origin = f * span + slot_in
            away = (source != f) | (origin != t)
            two = paired(origin, t)

            @pl.when(away & jnp.logical_not(two))
            def _():
                landed(source, slot_in, g).wait_recv()

            if both == 2:

                @pl.when(away & two & (lax.rem(g, 2) == 0))
                def _():
                    landed(source, slot_in, lax.div(g, both) * both, both).wait_recv()

            return c

        with jax.named_scope("await"):
            lax.fori_loop(0, PER_FRAME, await_one, 0)

    def unit(i, c):
        n = lax.div(i, n_fq)
        source = lax.rem(f + lax.rem(i, n_fq), n_fq)
        late = n - (turns - groups)
        first = n < ready
        last = (late >= ready) & (late >= 0)
        inward = first | last
        g = jnp.where(first, n, jnp.where(last, late, lax.rem(n - ready, groups)))
        m = jnp.where(inward, 0, 1 + lax.div(n - ready, groups))
        m = lax.rem(m + inner_frame(f, frames), frames)

        await_unit(source, m, g)
        transform(
            recv.at[source], m, g, chunk, tc, ts, hi, lhs,
            flat.at[:, source * groups + g], m * FFT_LO, frames * FFT_LO,
        )
        return c

    lax.fori_loop(0, (turns - 1) * n_fq, unit, 0)

    def await_last(i, c):
        await_unit(lax.rem(f + i, n_fq), inner_frame(f, frames), groups - 1)
        return c

    lax.fori_loop(0, n_fq, await_last, 0)
    with jax.named_scope("sent"):
        lax.fori_loop(0, groups, all_sent, 0)
        halo_copy(0, right).wait_send()
        halo_copy(1, left).wait_send()


def inner_frame(f, frames):
    return lax.rem(frames - 1 + f, frames)


def last_kernel(n_fq, y, recv, tc, ts, hi, out, tail, lhs, sems, tail_sems):
    f = lax.axis_index("freq")
    parts, blocks, chunk, frames = y.shape[:4]
    groups = blocks // n_fq
    mine = inner_frame(f, frames)
    copies = []
    for p in range(parts):
        for b in range(blocks):
            if b % groups < groups - 1:
                copies.append((y.at[p, b], out.at[p, b]))
            else:
                for j in range(1, frames):
                    m = lax.rem(mine + j, frames)
                    copies.append((y.at[p, b, :, m], out.at[p, b, :, m]))
    copies = [pltpu.make_async_copy(a, b, sems.at[i]) for i, (a, b) in enumerate(copies)]
    for c in copies:
        c.start()

    def tail_copy(p, source):
        return pltpu.make_async_copy(
            tail.at[source, p], out.at[p, source * groups + groups - 1, :, mine], tail_sems.at[p, source]
        )

    def unit(source, c):
        flat = tail.reshape(n_fq, parts, chunk * FFT_LO, FFT_HI)
        transform(
            recv.at[source], mine, groups - 1, chunk, tc, ts, hi, lhs, flat.at[source], 0, FFT_LO
        )
        for p in range(parts):
            tail_copy(p, source).start()
        return c

    lax.fori_loop(0, n_fq, unit, 0)
    for c in copies:
        c.wait()
    for source in range(n_fq):
        for p in range(parts):
            tail_copy(p, source).wait()


def shards(strengths, sample_cell, sample_frac):
    n_tm, n_fq = lax.axis_size("tm"), lax.axis_size("freq")
    parts, groups, channels, samples = strengths.shape
    span = n_tm // n_fq
    frames = span // PER_FRAME
    chunk = channels // n_tm
    rows = parts * chunk
    total = groups * n_tm * rows
    low = np.arange(FFT_LO)[:, None] * np.arange(FFT_HI)[None, :] * (2 * math.pi / FFTLEN)
    high = np.arange(FFT_HI)[:, None] * np.arange(FFT_HI)[None, :] % FFT_HI * (2 * math.pi / FFT_HI)
    hc, hs = np.cos(high), np.sin(high)
    full = np.block([[hc, -hs], [hs, hc]]).astype(np.float32) / math.sqrt(FFTLEN)
    vmem = pl.BlockSpec(memory_space=pltpu.VMEM)
    y_shape = (parts, n_fq * groups, chunk, frames, FFT_LO, FFT_HI)
    results = pl.pallas_call(
        functools.partial(main_kernel, n_tm, n_fq),
        out_shape=(
            pltpu.VMEM(y_shape, jnp.float32),
            pltpu.VMEM((n_fq, span, groups, SLABS, rows, LANES), jnp.bfloat16),
            pltpu.VMEM((FFT_LO, FFT_HI), jnp.float32),
            pltpu.VMEM((FFT_LO, FFT_HI), jnp.float32),
            pltpu.VMEM((2 * FFT_HI, 2 * FFT_HI), jnp.bfloat16),
        ),
        in_specs=[pl.BlockSpec(memory_space=pltpu.HBM)] * 6,
        out_specs=(vmem,) * 5,
        scratch_shapes=[
            pltpu.VMEM((parts, groups, channels, samples), jnp.bfloat16),
            pltpu.VMEM((samples // LANES, LANES), jnp.int32),
            pltpu.VMEM((samples // LANES, LANES), jnp.float32),
            pltpu.VMEM((samples, LANES), jnp.float32),
            pltpu.VMEM((samples, LANES), jnp.float32),
            pltpu.VMEM((samples, (SLABS + 1) * LANES), jnp.bfloat16),
            pltpu.VMEM((16, total), jnp.float32),
            pltpu.VMEM((LANES, total), jnp.float32),
            pltpu.VMEM((n_tm, groups, SLABS, rows, LANES), jnp.bfloat16),
            pltpu.VMEM((FFT_LO * chunk, 2 * FFT_HI), jnp.bfloat16),
            pltpu.SemaphoreType.DMA((5,)),
            pltpu.SemaphoreType.DMA((2 * groups,)),
            pltpu.SemaphoreType.DMA((2, groups)),
            pltpu.SemaphoreType.DMA((n_fq, span, groups)),
            pltpu.SemaphoreType.DMA((2,)),
            pltpu.SemaphoreType.DMA((2,)),
        ],
        compiler_params=pltpu.CompilerParams(
            collective_id=0, has_side_effects=True, vmem_limit_bytes=48 * 1024 * 1024
        ),
        name="grid_exchange_transform",
    )(
        strengths,
        sample_cell.reshape(samples // LANES, LANES),
        sample_frac.reshape(samples // LANES, LANES),
        jnp.asarray(np.cos(low), jnp.float32),
        jnp.asarray(np.sin(low), jnp.float32),
        jnp.asarray(full.astype(jnp.bfloat16)),
    )
    return pl.pallas_call(
        functools.partial(last_kernel, n_fq),
        out_shape=jax.ShapeDtypeStruct(y_shape, jnp.float32),
        in_specs=[vmem] * 5,
        out_specs=pl.BlockSpec(memory_space=pl.ANY),
        scratch_shapes=[
            pltpu.VMEM((n_fq, parts, chunk, FFT_LO, FFT_HI), jnp.float32),
            pltpu.VMEM((FFT_LO * chunk, 2 * FFT_HI), jnp.bfloat16),
            pltpu.SemaphoreType.DMA((parts * n_fq * groups * frames,)),
            pltpu.SemaphoreType.DMA((parts, n_fq)),
        ],
        compiler_params=pltpu.CompilerParams(vmem_limit_bytes=16 * 1024 * 1024),
        name="last_units_write",
    )(*results)


def solution(mesh):
    placed = (P(None, "freq", None, "tm"), P("tm"), P("tm"))
    return jax.shard_map(
        shards,
        mesh=mesh,
        in_specs=placed,
        out_specs=P(None, None, "tm", "freq", None, None),
        check_vma=False,
    )
```

```python
import functools
import math

import jax
import jax.numpy as jnp
import numpy as np
from jax import lax
from jax.experimental import pallas as pl
from jax.experimental.pallas import tpu as pltpu
from jax.sharding import PartitionSpec as P

TAPS = 8
HALF = TAPS // 2
GRID_DEV = 1024
FFT_LO = 32
FFT_HI = 128
FFTLEN = 4096
SHARP = 0.3
MESH = pl.DeviceIdType.MESH
LANES = 128
SLABS = GRID_DEV // LANES
INNER = SLABS - 2
PER_FRAME = FFTLEN // GRID_DEV
EARLY = 3
FIRST = ((0, 2), (2, 4))
PLACE = [INNER] + list(range(INNER)) + [INNER + 1]


def fft_list(re, im):
    n = len(re)
    if n == 1:
        return re, im
    er, ei = fft_list(re[0::2], im[0::2])
    orr, oi = fft_list(re[1::2], im[1::2])
    out_r, out_i = [None] * n, [None] * n
    for k in range(n // 2):
        c, s = math.cos(2 * math.pi * k / n), math.sin(2 * math.pi * k / n)
        a, b = orr[k], oi[k]
        if k == 0:
            tr, ti = a, b
        elif 4 * k == n:
            tr, ti = b, -a
        elif 8 * k == n:
            tr, ti = (a + b) * c, (b - a) * c
        elif 8 * k == 3 * n:
            tr, ti = (b - a) * s, -(a + b) * s
        else:
            tr, ti = a * c + b * s, b * c - a * s
        out_r[k], out_i[k] = er[k] + tr, ei[k] + ti
        out_r[k + n // 2], out_i[k + n // 2] = er[k] - tr, ei[k] - ti
    return out_r, out_i


def sequence(pairs):
    return [(far, pair, core) for pair in reversed(range(pairs)) for core in range(2) for far in (1, 0)]


def transform(blocks, m, g, chunk, tc, ts, hi, lhs, out, start, stride):
    re, im = [], []
    for n in range(FFT_LO):
        tile = blocks[m * PER_FRAME + n // SLABS, g, PLACE[n % SLABS]]
        re.append(tile[:chunk].astype(jnp.float32))
        im.append(tile[chunk:].astype(jnp.float32))
    re, im = fft_list(re, im)
    for a in range(FFT_LO):
        cc = tc[a : a + 1, :]
        ss = ts[a : a + 1, :]
        at = pl.ds(a * chunk, chunk)
        lhs[at, :FFT_HI] = (re[a] * cc + im[a] * ss).astype(jnp.bfloat16)
        lhs[at, FFT_HI:] = (im[a] * cc - re[a] * ss).astype(jnp.bfloat16)
    y = jnp.dot(lhs[...], hi[...], preferred_element_type=jnp.float32)
    for a in range(FFT_LO):
        for p in range(2):
            out[p, pl.ds(start + a, chunk, stride=stride), :] = y[
                a * chunk : (a + 1) * chunk, p * FFT_HI : (p + 1) * FFT_HI
            ]


def main_kernel(
    n_tm, n_fq, strengths, cell_hbm, frac_hbm, tc_hbm, ts_hbm, hi_hbm, y, recv, tc, ts, hi,
    xv, cell, frac, cols, fracs, table, edge_out, halo, src, lhs,
    small, load, send, arrive, halo_send, halo_arrive,
):
    t = lax.axis_index("tm")
    f = lax.axis_index("freq")
    parts, groups, channels, samples = xv.shape
    chunk = channels // n_tm
    rows = src.shape[3]
    wide = channels // 2
    both = 2 if groups % 2 == 0 else 1
    span = n_tm // n_fq
    frames = span // PER_FRAME
    slot = lax.rem(t, span)
    home = lax.div(t, span)
    half = n_tm // 2
    block = half * rows
    upper = lax.div(t, half)
    quarter = lax.div(t, n_tm // 4)
    outer = (quarter == 0) | (quarter == 3)
    right = lax.rem(t + 1, n_tm)
    left = lax.rem(t + n_tm - 1, n_tm)
    steps = 2 * groups
    early = min(EARLY, steps)
    keep = home == f

    def order(k):
        ahead = (k == 0) | ((lax.rem(k, 2) == 1) & (k < steps - 1))
        far = jnp.where(outer, k >= groups, ahead)
        inward = jnp.where(ahead, lax.div(k + 1, 2), lax.div(k - 1, 2))
        side = jnp.where(far, 1 - upper, upper)
        return side, jnp.where(outer, lax.rem(k, groups), inward)

    constants = [
        pltpu.make_async_copy(a, b, small.at[i])
        for i, (a, b) in enumerate(
            ((cell_hbm, cell), (frac_hbm, frac), (tc_hbm, tc), (ts_hbm, ts), (hi_hbm, hi))
        )
    ]
    for i in range(2):
        constants[i].start()

    barrier = pltpu.get_barrier_semaphore()

    def greet(i, c):
        origin = f * span + lax.rem(slot + 1 + i, span)

        def one(j, c):
            other = lax.rem(f + j, n_fq)

            @pl.when((origin != t) | (other != f))
            def _():
                pl.semaphore_signal(barrier, inc=1, device_id=(origin, other), device_id_type=MESH)

            return c

        return lax.fori_loop(0, n_fq, one, c)

    with jax.named_scope("greet"):
        lax.fori_loop(0, span, greet, 0)
        for peer in (left, right):
            pl.semaphore_signal(barrier, inc=1, device_id=(peer, f), device_id_type=MESH)

    def fetch(k):
        side, g = order(k)
        at = (slice(None), g, pl.ds(pl.multiple_of(side * wide, wide), wide))
        return pltpu.make_async_copy(strengths.at[at], xv.at[at], load.at[k])

    fetch(0).start()

    with jax.named_scope('fetch'):
        for k in range(1, steps):
            fetch(k).start()

    base = t * GRID_DEV
    with jax.named_scope('cw'):
        constants[0].wait()
        constants[1].wait()
    for i in range(samples // LANES):
        at = pl.ds(i * LANES, LANES)
        local = (cell[i : i + 1, :] - base).astype(jnp.float32)
        cols[at, :] = jnp.broadcast_to(local, (LANES, LANES)).T
        fracs[at, :] = jnp.broadcast_to(frac[i : i + 1, :], (LANES, LANES)).T
    lane = lax.broadcasted_iota(jnp.int32, (LANES, LANES), 1)

    def build(place, columns):
        def part(i, c):
            at = pl.ds(pl.multiple_of(i * LANES, LANES), LANES)
            d = columns - cols[at, :]
            u = d - fracs[at, :]
            w = jnp.exp(-SHARP * (u * u))
            inside = jnp.abs(d - 0.5) < float(HALF)
            table[at, place * LANES : (place + 1) * LANES] = jnp.where(inside, w, 0.0).astype(jnp.bfloat16)
            return c

        lax.fori_loop(0, samples // LANES, part, 0, unroll=4)

    def slab_columns(j):
        return (lane + j * LANES).astype(jnp.float32)

    def operand(k):
        side, g = order(k)
        at = pl.ds(pl.multiple_of(side * wide, wide), wide)
        return xv[:, g, at, :].reshape(block, samples)

    def product(k, first, count):
        return jnp.dot(
            operand(k),
            table[:, first * LANES : (first + count) * LANES],
            preferred_element_type=jnp.float32,
        )

    def put(k, first, pieces):
        side, g = order(k)
        for j, part in enumerate(pieces):
            part = part.astype(jnp.bfloat16)
            for i in range(half):
                for p in range(parts):
                    start = p * wide + i * chunk
                    src[side * half + i, g, first + j, p * chunk : (p + 1) * chunk] = part[start : start + chunk]

    def slabs(acc):
        return [acc[:, j : j + LANES] for j in range(0, acc.shape[1], LANES)]

    def with_halo(k, low, high):
        side, g = order(k)
        at = pl.ds(pl.multiple_of(g * channels + side * wide, LANES), wide)
        empty = jnp.zeros((LANES - 2 * HALF, wide), jnp.float32)
        outside = jnp.concatenate(
            [
                jnp.concatenate(
                    [halo[0, p * HALF : (p + 1) * HALF, at], empty, halo[1, p * HALF : (p + 1) * HALF, at]]
                ).T
                for p in range(parts)
            ]
        )
        spot = lax.broadcasted_iota(jnp.int32, (block, LANES), 1)
        return [
            low + jnp.where(spot < LANES // 2, outside, 0.0),
            high + jnp.where(spot >= LANES // 2, outside, 0.0),
        ]

    def copy_out(d, g, first, count, pair=1):
        part = (pl.ds(g, pair), pl.ds(first, count))
        return pltpu.make_async_remote_copy(
            src_ref=src.at[(d,) + part],
            dst_ref=recv.at[(f, slot) + part],
            send_sem=send.at[lax.div(d, half), g],
            recv_sem=arrive.at[f, slot, g],
            device_id=(d, home),
            device_id_type=MESH,
        )

    pairs = n_tm // 8
    pair_at = lax.rem(lax.div(t, 2), pairs)
    core_at = lax.rem(t, 2)

    def target(side, far, pair, core):
        across = lax.rem(side + 1 + far, 2)
        return side * half + across * (half // 2) + lax.rem(pair_at + pair, pairs) * 2 + lax.rem(core_at + core, 2)


    def send_step(k, first, count, pair=1):
        side, g = order(k)
        for far, pair_by, core_by in sequence(pairs):
            d = target(side, far, pair_by, core_by)

            @pl.when((d != t) | (home != f))
            def _():
                copy_out(d, g - (pair - 1), first, count, pair).start()

    fetch(0).wait()
    with jax.named_scope("first"):
        for first, count in FIRST:
            for j in range(first, first + count):
                build(j, slab_columns(1 + j))
            put(0, first, slabs(product(0, first, count)))
            if first == 0:
                with jax.named_scope('bar'):
                    pl.semaphore_wait(barrier, jnp.where(keep, n_tm + 1, n_tm + 2))
            send_step(0, first, count)
            if first == 0:
                for i in range(2, 5):
                    constants[i].start()

    beyond = jnp.where(
        lane < HALF, lane + GRID_DEV, jnp.where(lane < 2 * HALF, lane - 2 * HALF, -GRID_DEV)
    ).astype(jnp.float32)

    def edges(g, c):
        acc = jnp.dot(
            xv[:, g].reshape(2 * block, samples),
            table[:, SLABS * LANES :],
            preferred_element_type=jnp.float32,
        )
        across = acc.T[: 2 * HALF]
        at = pl.ds(pl.multiple_of(g * channels, LANES), channels)
        for side in range(2):
            edge_out[side, :, at] = jnp.concatenate(
                [
                    across[side * HALF : (side + 1) * HALF, p * channels : (p + 1) * channels]
                    for p in range(parts)
                ]
            )
        return c

    with jax.named_scope("edges"):
        build(SLABS, beyond)
        for k in range(1, steps):
            fetch(k).wait()
        lax.fori_loop(0, groups, edges, 0)

    def halo_copy(i, peer):
        return pltpu.make_async_remote_copy(
            src_ref=edge_out.at[i],
            dst_ref=halo.at[i],
            send_sem=halo_send.at[i],
            recv_sem=halo_arrive.at[i],
            device_id=(peer, f),
            device_id_type=MESH,
        )

    halo_copy(0, right).start()
    halo_copy(1, left).start()

    def early_step(k, c):
        put(k, 0, slabs(product(k, 0, INNER)))
        send_step(k, 0, INNER)
        return c

    with jax.named_scope("early"):
        lax.fori_loop(1, early, early_step, 0)
        build(INNER, slab_columns(0))
        build(INNER + 1, slab_columns(SLABS - 1))
    with jax.named_scope("halo_wait"):
        halo_copy(0, right).wait_recv()
        halo_copy(1, left).wait_recv()

    def early_edges(k, c):
        put(k, INNER, with_halo(k, *slabs(product(k, INNER, 2))))
        send_step(k, INNER, 2)
        return c

    def late_step(k, c):
        pieces = slabs(product(k, 0, SLABS))
        put(k, 0, pieces[:INNER] + with_halo(k, *pieces[INNER:]))
        if both == 1:
            send_step(k, 0, SLABS)
        else:
            in_pairs = outer & (k >= groups)

            @pl.when(in_pairs & (lax.rem(k, 2) == 1))
            def _():
                send_step(k, 0, SLABS, both)

            @pl.when(jnp.logical_not(in_pairs))
            def _():
                send_step(k, 0, SLABS)

        return c

    with jax.named_scope("early_edges"):
        lax.fori_loop(0, early, early_edges, 0)
    with jax.named_scope("late"):
        lax.fori_loop(early, steps, late_step, 0)

    @pl.when(keep)
    def _():
        def own(g, c):
            recv[f, slot, g] = src[t, g]
            return c

        lax.fori_loop(0, groups, own, 0)

    def landed(source, s, g, pair=1):
        return pltpu.make_async_remote_copy(
            src_ref=src.at[0, pl.ds(g, pair)],
            dst_ref=recv.at[source, s, pl.ds(g, pair)],
            send_sem=send.at[0, 0],
            recv_sem=arrive.at[source, s, g],
            device_id=(t, f),
            device_id_type=MESH,
        )

    def is_outer(index):
        q = lax.div(index, n_tm // 4)
        return (q == 0) | (q == 3)

    def paired(origin, d):
        return is_outer(origin) & (lax.div(origin, half) != lax.div(d, half)) & (both == 2)

    for i in range(2, 5):
        constants[i].wait()
    flat = y.reshape(2, n_fq * groups, chunk * frames * FFT_LO, FFT_HI)
    ready = min(2, groups)
    turns = frames * groups

    def sent(side, g, count, pair=1):
        part = src.at[pl.ds(side * half, count), pl.ds(g, pair)]
        pltpu.make_async_remote_copy(
            src_ref=part,
            dst_ref=part,
            send_sem=send.at[side, g],
            recv_sem=arrive.at[0, 0, 0],
            device_id=(right, f),
            device_id_type=MESH,
        ).wait_send()

    def all_sent(g, c):
        @pl.when(keep)
        def _():
            sent(upper, g, half - 1)

        @pl.when(jnp.logical_not(keep))
        def _():
            sent(upper, g, half)

        if both == 1:
            sent(1 - upper, g, half)
        else:

            @pl.when(jnp.logical_not(outer))
            def _():
                sent(1 - upper, g, half)

            @pl.when(outer & (lax.rem(g, 2) == 0))
            def _():
                sent(1 - upper, g, half, both)

        return c

    def await_unit(source, m, g):
        def await_one(s, c):
            slot_in = m * PER_FRAME + s
            origin = f * span + slot_in
            away = (source != f) | (origin != t)
            two = paired(origin, t)

            @pl.when(away & jnp.logical_not(two))
            def _():
                landed(source, slot_in, g).wait_recv()

            if both == 2:

                @pl.when(away & two & (lax.rem(g, 2) == 0))
                def _():
                    landed(source, slot_in, lax.div(g, both) * both, both).wait_recv()

            return c

        with jax.named_scope("await"):
            lax.fori_loop(0, PER_FRAME, await_one, 0)

    def unit(i, c):
        n = lax.div(i, n_fq)
        source = lax.rem(f + lax.rem(i, n_fq), n_fq)
        late = n - (turns - groups)
        first = n < ready
        last = (late >= ready) & (late >= 0)
        inward = first | last
        g = jnp.where(first, n, jnp.where(last, late, lax.rem(n - ready, groups)))
        m = jnp.where(inward, 0, 1 + lax.div(n - ready, groups))
        m = lax.rem(m + inner_frame(f, frames), frames)

        await_unit(source, m, g)
        transform(
            recv.at[source], m, g, chunk, tc, ts, hi, lhs,
            flat.at[:, source * groups + g], m * FFT_LO, frames * FFT_LO,
        )
        return c

    lax.fori_loop(0, (turns - 1) * n_fq, unit, 0)

    def await_last(i, c):
        await_unit(lax.rem(f + i, n_fq), inner_frame(f, frames), groups - 1)
        return c

    lax.fori_loop(0, n_fq, await_last, 0)
    with jax.named_scope("sent"):
        lax.fori_loop(0, groups, all_sent, 0)
        halo_copy(0, right).wait_send()
        halo_copy(1, left).wait_send()


def inner_frame(f, frames):
    return lax.rem(frames - 1 + f, frames)


def last_kernel(n_fq, y, recv, tc, ts, hi, out, tail, lhs, sems, tail_sems):
    f = lax.axis_index("freq")
    parts, blocks, chunk, frames = y.shape[:4]
    groups = blocks // n_fq
    mine = inner_frame(f, frames)
    copies = []
    for p in range(parts):
        for b in range(blocks):
            if b % groups < groups - 1:
                copies.append((y.at[p, b], out.at[p, b]))
            else:
                for j in range(1, frames):
                    m = lax.rem(mine + j, frames)
                    copies.append((y.at[p, b, :, m], out.at[p, b, :, m]))
    copies = [pltpu.make_async_copy(a, b, sems.at[i]) for i, (a, b) in enumerate(copies)]
    for c in copies:
        c.start()

    def tail_copy(p, source):
        return pltpu.make_async_copy(
            tail.at[source, p], out.at[p, source * groups + groups - 1, :, mine], tail_sems.at[p, source]
        )

    def unit(source, c):
        flat = tail.reshape(n_fq, parts, chunk * FFT_LO, FFT_HI)
        transform(
            recv.at[source], mine, groups - 1, chunk, tc, ts, hi, lhs, flat.at[source], 0, FFT_LO
        )
        for p in range(parts):
            tail_copy(p, source).start()
        return c

    lax.fori_loop(0, n_fq, unit, 0)
    for c in copies:
        c.wait()
    for source in range(n_fq):
        for p in range(parts):
            tail_copy(p, source).wait()


def shards(strengths, sample_cell, sample_frac):
    n_tm, n_fq = lax.axis_size("tm"), lax.axis_size("freq")
    parts, groups, channels, samples = strengths.shape
    span = n_tm // n_fq
    frames = span // PER_FRAME
    chunk = channels // n_tm
    rows = parts * chunk
    total = groups * n_tm * rows
    low = np.arange(FFT_LO)[:, None] * np.arange(FFT_HI)[None, :] * (2 * math.pi / FFTLEN)
    high = np.arange(FFT_HI)[:, None] * np.arange(FFT_HI)[None, :] % FFT_HI * (2 * math.pi / FFT_HI)
    hc, hs = np.cos(high), np.sin(high)
    full = np.block([[hc, -hs], [hs, hc]]).astype(np.float32) / math.sqrt(FFTLEN)
    vmem = pl.BlockSpec(memory_space=pltpu.VMEM)
    y_shape = (parts, n_fq * groups, chunk, frames, FFT_LO, FFT_HI)
    results = pl.pallas_call(
        functools.partial(main_kernel, n_tm, n_fq),
        out_shape=(
            pltpu.VMEM(y_shape, jnp.float32),
            pltpu.VMEM((n_fq, span, groups, SLABS, rows, LANES), jnp.bfloat16),
            pltpu.VMEM((FFT_LO, FFT_HI), jnp.float32),
            pltpu.VMEM((FFT_LO, FFT_HI), jnp.float32),
            pltpu.VMEM((2 * FFT_HI, 2 * FFT_HI), jnp.bfloat16),
        ),
        in_specs=[pl.BlockSpec(memory_space=pltpu.HBM)] * 6,
        out_specs=(vmem,) * 5,
        scratch_shapes=[
            pltpu.VMEM((parts, groups, channels, samples), jnp.bfloat16),
            pltpu.VMEM((samples // LANES, LANES), jnp.int32),
            pltpu.VMEM((samples // LANES, LANES), jnp.float32),
            pltpu.VMEM((samples, LANES), jnp.float32),
            pltpu.VMEM((samples, LANES), jnp.float32),
            pltpu.VMEM((samples, (SLABS + 1) * LANES), jnp.bfloat16),
            pltpu.VMEM((2, parts * HALF, total // parts), jnp.float32),
            pltpu.VMEM((2, parts * HALF, total // parts), jnp.float32),
            pltpu.VMEM((n_tm, groups, SLABS, rows, LANES), jnp.bfloat16),
            pltpu.VMEM((FFT_LO * chunk, 2 * FFT_HI), jnp.bfloat16),
            pltpu.SemaphoreType.DMA((5,)),
            pltpu.SemaphoreType.DMA((2 * groups,)),
            pltpu.SemaphoreType.DMA((2, groups)),
            pltpu.SemaphoreType.DMA((n_fq, span, groups)),
            pltpu.SemaphoreType.DMA((2,)),
            pltpu.SemaphoreType.DMA((2,)),
        ],
        compiler_params=pltpu.CompilerParams(
            collective_id=0, has_side_effects=True, vmem_limit_bytes=48 * 1024 * 1024
        ),
        name="grid_exchange_transform",
    )(
        strengths,
        sample_cell.reshape(samples // LANES, LANES),
        sample_frac.reshape(samples // LANES, LANES),
        jnp.asarray(np.cos(low), jnp.float32),
        jnp.asarray(np.sin(low), jnp.float32),
        jnp.asarray(full.astype(jnp.bfloat16)),
    )
    return pl.pallas_call(
        functools.partial(last_kernel, n_fq),
        out_shape=jax.ShapeDtypeStruct(y_shape, jnp.float32),
        in_specs=[vmem] * 5,
        out_specs=pl.BlockSpec(memory_space=pl.ANY),
        scratch_shapes=[
            pltpu.VMEM((n_fq, parts, chunk, FFT_LO, FFT_HI), jnp.float32),
            pltpu.VMEM((FFT_LO * chunk, 2 * FFT_HI), jnp.bfloat16),
            pltpu.SemaphoreType.DMA((parts * n_fq * groups * frames,)),
            pltpu.SemaphoreType.DMA((parts, n_fq)),
        ],
        compiler_params=pltpu.CompilerParams(vmem_limit_bytes=16 * 1024 * 1024),
        name="last_units_write",
    )(*results)


def solution(mesh):
    placed = (P(None, "freq", None, "tm"), P("tm"), P("tm"))
    return jax.shard_map(
        shards,
        mesh=mesh,
        in_specs=placed,
        out_specs=P(None, None, "tm", "freq", None, None),
        check_vma=False,
    )
```

```python
import functools
import math

import jax
import jax.numpy as jnp
import numpy as np
from jax import lax
from jax.experimental import pallas as pl
from jax.experimental.pallas import tpu as pltpu
from jax.sharding import PartitionSpec as P

TAPS = 8
HALF = TAPS // 2
GRID_DEV = 1024
FFT_LO = 32
FFT_HI = 128
FFTLEN = 4096
SHARP = 0.3
MESH = pl.DeviceIdType.MESH
LANES = 128
SLABS = GRID_DEV // LANES
INNER = SLABS - 2
PER_FRAME = FFTLEN // GRID_DEV
EARLY = 3
FIRST = ((0, 2), (2, 2), (4, 2))
PLACE = [INNER] + list(range(INNER)) + [INNER + 1]


def fft_list(re, im):
    n = len(re)
    if n == 1:
        return re, im
    er, ei = fft_list(re[0::2], im[0::2])
    orr, oi = fft_list(re[1::2], im[1::2])
    out_r, out_i = [None] * n, [None] * n
    for k in range(n // 2):
        c, s = math.cos(2 * math.pi * k / n), math.sin(2 * math.pi * k / n)
        a, b = orr[k], oi[k]
        if k == 0:
            tr, ti = a, b
        elif 4 * k == n:
            tr, ti = b, -a
        elif 8 * k == n:
            tr, ti = (a + b) * c, (b - a) * c
        elif 8 * k == 3 * n:
            tr, ti = (b - a) * s, -(a + b) * s
        else:
            tr, ti = a * c + b * s, b * c - a * s
        out_r[k], out_i[k] = er[k] + tr, ei[k] + ti
        out_r[k + n // 2], out_i[k + n // 2] = er[k] - tr, ei[k] - ti
    return out_r, out_i


def sequence(pairs):
    return [(far, pair, core) for pair in reversed(range(pairs)) for core in range(2) for far in (1, 0)]


def transform(blocks, m, g, chunk, tc, ts, hi, lhs, out, start, stride):
    re, im = [], []
    for n in range(FFT_LO):
        tile = blocks[m * PER_FRAME + n // SLABS, g, PLACE[n % SLABS]]
        re.append(tile[:chunk].astype(jnp.float32))
        im.append(tile[chunk:].astype(jnp.float32))
    re, im = fft_list(re, im)
    for a in range(FFT_LO):
        cc = tc[a : a + 1, :]
        ss = ts[a : a + 1, :]
        at = pl.ds(a * chunk, chunk)
        lhs[at, :FFT_HI] = (re[a] * cc + im[a] * ss).astype(jnp.bfloat16)
        lhs[at, FFT_HI:] = (im[a] * cc - re[a] * ss).astype(jnp.bfloat16)
    y = jnp.dot(lhs[...], hi[...], preferred_element_type=jnp.float32)
    for a in range(FFT_LO):
        for p in range(2):
            out[p, pl.ds(start + a, chunk, stride=stride), :] = y[
                a * chunk : (a + 1) * chunk, p * FFT_HI : (p + 1) * FFT_HI
            ]


def main_kernel(
    n_tm, n_fq, strengths, cell_hbm, frac_hbm, tc_hbm, ts_hbm, hi_hbm, y, recv, tc, ts, hi,
    xv, cell, frac, cols, fracs, table, edge_out, halo, src, lhs,
    small, load, send, arrive, halo_send, halo_arrive, ready,
):
    t = lax.axis_index("tm")
    f = lax.axis_index("freq")
    parts, groups, channels, samples = xv.shape
    chunk = channels // n_tm
    rows = src.shape[3]
    wide = channels // 2
    both = groups
    span = n_tm // n_fq
    frames = span // PER_FRAME
    slot = lax.rem(t, span)
    home = lax.div(t, span)
    half = n_tm // 2
    block = half * rows
    upper = lax.div(t, half)
    quarter = lax.div(t, n_tm // 4)
    outer = (quarter == 0) | (quarter == 3)
    right = lax.rem(t + 1, n_tm)
    left = lax.rem(t + n_tm - 1, n_tm)
    steps = 2 * groups
    early = min(EARLY, steps)
    keep = home == f

    def order(k):
        ahead = (k == 0) | ((lax.rem(k, 2) == 1) & (k < steps - 1))
        far = jnp.where(outer, k >= groups, ahead)
        inward = jnp.where(ahead, lax.div(k + 1, 2), lax.div(k - 1, 2))
        side = jnp.where(far, 1 - upper, upper)
        return side, jnp.where(outer, lax.rem(k, groups), inward)

    constants = [
        pltpu.make_async_copy(a, b, small.at[i])
        for i, (a, b) in enumerate(
            ((cell_hbm, cell), (frac_hbm, frac), (tc_hbm, tc), (ts_hbm, ts), (hi_hbm, hi))
        )
    ]
    for i in range(2):
        constants[i].start()

    barrier = pltpu.get_barrier_semaphore()
    size = n_tm // 4
    mate = jnp.where((quarter == 0) | (quarter == 2), t + size, t - size)

    def outer_of(index):
        q = lax.div(index, size)
        return jnp.where(q == 1, index - size, jnp.where(q == 2, index + size, index))

    def greet_one(tm, freq):
        pl.semaphore_signal(barrier, inc=1, device_id=(tm, freq), device_id_type=MESH)

    def greet(i, c):
        origin = f * span + lax.rem(slot + 1 + i, span)
        host = outer_of(origin)
        facing = jnp.logical_not(outer) & (lax.div(origin, size) == 3 - quarter)

        def one(j, c):
            other = lax.rem(f + j, n_fq)

            @pl.when(facing)
            def _():
                greet_one(origin, other)

            @pl.when((host != t) | (other != f))
            def _():
                greet_one(host, other)

            return c

        return lax.fori_loop(0, n_fq, one, c)

    lax.fori_loop(0, span, greet, 0)
    greet_one(outer_of(left), f)
    greet_one(outer_of(right), f)

    @pl.when(jnp.logical_not(outer))
    def _():
        greet_one(mate, f)

    def greeted():
        own = jnp.where(keep, n_tm - 1, n_tm)
        others = jnp.where(lax.div(mate, span) == f, n_tm - 1, n_tm)
        pl.semaphore_wait(barrier, jnp.where(outer, own + others + 5, size))

        @pl.when(outer)
        def _():
            pl.semaphore_signal(ready, inc=1, device_id=(mate, f), device_id_type=MESH)

    def fetch(k):
        side, g = order(k)
        at = (slice(None), g, pl.ds(pl.multiple_of(side * wide, wide), wide))
        return pltpu.make_async_copy(strengths.at[at], xv.at[at], load.at[k])

    fetch(0).start()

    for k in range(1, steps):
        fetch(k).start()

    base = t * GRID_DEV
    constants[0].wait()
    constants[1].wait()
    for i in range(samples // LANES):
        at = pl.ds(i * LANES, LANES)
        local = (cell[i : i + 1, :] - base).astype(jnp.float32)
        cols[at, :] = jnp.broadcast_to(local, (LANES, LANES)).T
        fracs[at, :] = jnp.broadcast_to(frac[i : i + 1, :], (LANES, LANES)).T
    lane = lax.broadcasted_iota(jnp.int32, (LANES, LANES), 1)

    def build(place, columns):
        def part(i, c):
            at = pl.ds(pl.multiple_of(i * LANES, LANES), LANES)
            d = columns - cols[at, :]
            u = d - fracs[at, :]
            w = jnp.exp(-SHARP * (u * u))
            inside = jnp.abs(d - 0.5) < float(HALF)
            table[at, place * LANES : (place + 1) * LANES] = jnp.where(inside, w, 0.0).astype(jnp.bfloat16)
            return c

        lax.fori_loop(0, samples // LANES, part, 0, unroll=4)

    def slab_columns(j):
        return (lane + j * LANES).astype(jnp.float32)

    def operand(k):
        side, g = order(k)
        at = pl.ds(pl.multiple_of(side * wide, wide), wide)
        return xv[:, g, at, :].reshape(block, samples)

    def product(k, first, count):
        return jnp.dot(
            operand(k),
            table[:, first * LANES : (first + count) * LANES],
            preferred_element_type=jnp.float32,
        )

    def put(k, first, pieces):
        side, g = order(k)
        for j, part in enumerate(pieces):
            part = part.astype(jnp.bfloat16)
            for i in range(half):
                for p in range(parts):
                    start = p * wide + i * chunk
                    src[side * half + i, g, first + j, p * chunk : (p + 1) * chunk] = part[start : start + chunk]

    def slabs(acc):
        return [acc[:, j : j + LANES] for j in range(0, acc.shape[1], LANES)]

    def with_halo(k, low, high):
        side, g = order(k)
        at = pl.ds(pl.multiple_of(g * channels + side * wide, LANES), wide)
        empty = jnp.zeros((LANES - 2 * HALF, wide), jnp.float32)
        outside = jnp.concatenate(
            [
                jnp.concatenate(
                    [halo[0, p * HALF : (p + 1) * HALF, at], empty, halo[1, p * HALF : (p + 1) * HALF, at]]
                ).T
                for p in range(parts)
            ]
        )
        spot = lax.broadcasted_iota(jnp.int32, (block, LANES), 1)
        return [
            low + jnp.where(spot < LANES // 2, outside, 0.0),
            high + jnp.where(spot >= LANES // 2, outside, 0.0),
        ]

    def copy_out(d, g, first, count, pair=1):
        part = (pl.ds(g, pair), pl.ds(first, count))
        return pltpu.make_async_remote_copy(
            src_ref=src.at[(d,) + part],
            dst_ref=recv.at[(f, slot) + part],
            send_sem=send.at[lax.div(d, half), g],
            recv_sem=arrive.at[f, slot, g],
            device_id=(d, home),
            device_id_type=MESH,
        )

    pairs = n_tm // 8
    pair_at = lax.rem(lax.div(t, 2), pairs)
    core_at = lax.rem(t, 2)

    def target(side, far, pair, core):
        across = lax.rem(side + 1 + far, 2)
        return side * half + across * (half // 2) + lax.rem(pair_at + pair, pairs) * 2 + lax.rem(core_at + core, 2)


    def send_step(k, first, count, pair=1, which=(0, 1)):
        side, g = order(k)
        for far, pair_by, core_by in sequence(pairs):
            if far not in which:
                continue
            d = target(side, far, pair_by, core_by)

            @pl.when((d != t) | (home != f))
            def _():
                copy_out(d, g - (pair - 1), first, count, pair).start()

    fetch(0).wait()
    with jax.named_scope("first"):
        for first, count in FIRST:
            for j in range(first, first + count):
                build(j, slab_columns(1 + j))
            put(0, first, slabs(product(0, first, count)))
            if first == 0:
                with jax.named_scope("bar"):
                    greeted()
            send_step(0, first, count, which=(0,))
            if first == 0:
                for i in range(2, 5):
                    constants[i].start()

        with jax.named_scope("ready"):

            @pl.when(jnp.logical_not(outer))
            def _():
                pl.semaphore_wait(ready, 1)

        send_step(0, 0, INNER, which=(1,))

    beyond = jnp.where(
        lane < HALF, lane + GRID_DEV, jnp.where(lane < 2 * HALF, lane - 2 * HALF, -GRID_DEV)
    ).astype(jnp.float32)

    def edges(g, c):
        acc = jnp.dot(
            xv[:, g].reshape(2 * block, samples),
            table[:, SLABS * LANES :],
            preferred_element_type=jnp.float32,
        )
        across = acc.T[: 2 * HALF]
        at = pl.ds(pl.multiple_of(g * channels, LANES), channels)
        for side in range(2):
            edge_out[side, :, at] = jnp.concatenate(
                [
                    across[side * HALF : (side + 1) * HALF, p * channels : (p + 1) * channels]
                    for p in range(parts)
                ]
            )
        return c

    with jax.named_scope("edges"):
        build(SLABS, beyond)
        for k in range(1, steps):
            fetch(k).wait()
        lax.fori_loop(0, groups, edges, 0)

    def halo_copy(i, peer):
        return pltpu.make_async_remote_copy(
            src_ref=edge_out.at[i],
            dst_ref=halo.at[i],
            send_sem=halo_send.at[i],
            recv_sem=halo_arrive.at[i],
            device_id=(peer, f),
            device_id_type=MESH,
        )

    halo_copy(0, right).start()
    halo_copy(1, left).start()

    def early_step(k, c):
        put(k, 0, slabs(product(k, 0, INNER)))
        send_step(k, 0, INNER)
        return c

    with jax.named_scope("early"):
        lax.fori_loop(1, early, early_step, 0)
        build(INNER, slab_columns(0))
        build(INNER + 1, slab_columns(SLABS - 1))
    with jax.named_scope("halo_wait"):
        halo_copy(0, right).wait_recv()
        halo_copy(1, left).wait_recv()

    def early_edges(k, c):
        put(k, INNER, with_halo(k, *slabs(product(k, INNER, 2))))
        send_step(k, INNER, 2)
        return c

    def late_step(k, c):
        pieces = slabs(product(k, 0, SLABS))
        put(k, 0, pieces[:INNER] + with_halo(k, *pieces[INNER:]))
        if both == 1:
            send_step(k, 0, SLABS)
        else:
            in_pairs = outer & (k >= groups)

            @pl.when(in_pairs & (lax.rem(k, both) == both - 1))
            def _():
                send_step(k, 0, SLABS, both)

            @pl.when(jnp.logical_not(in_pairs))
            def _():
                send_step(k, 0, SLABS)

        return c

    with jax.named_scope("early_edges"):
        lax.fori_loop(0, early, early_edges, 0)
    with jax.named_scope("late"):
        lax.fori_loop(early, steps, late_step, 0)

    @pl.when(keep)
    def _():
        def own(g, c):
            recv[f, slot, g] = src[t, g]
            return c

        lax.fori_loop(0, groups, own, 0)

    def landed(source, s, g, pair=1):
        return pltpu.make_async_remote_copy(
            src_ref=src.at[0, pl.ds(g, pair)],
            dst_ref=recv.at[source, s, pl.ds(g, pair)],
            send_sem=send.at[0, 0],
            recv_sem=arrive.at[source, s, g],
            device_id=(t, f),
            device_id_type=MESH,
        )

    def is_outer(index):
        q = lax.div(index, n_tm // 4)
        return (q == 0) | (q == 3)

    def paired(origin, d):
        return is_outer(origin) & (lax.div(origin, half) != lax.div(d, half)) & (both > 1)

    for i in range(2, 5):
        constants[i].wait()
    flat = y.reshape(2, n_fq * groups, chunk * frames * FFT_LO, FFT_HI)
    ready = min(2, groups)
    turns = frames * groups

    def sent(side, g, count, pair=1):
        part = src.at[pl.ds(side * half, count), pl.ds(g, pair)]
        pltpu.make_async_remote_copy(
            src_ref=part,
            dst_ref=part,
            send_sem=send.at[side, g],
            recv_sem=arrive.at[0, 0, 0],
            device_id=(right, f),
            device_id_type=MESH,
        ).wait_send()

    def all_sent(g, c):
        @pl.when(keep)
        def _():
            sent(upper, g, half - 1)

        @pl.when(jnp.logical_not(keep))
        def _():
            sent(upper, g, half)

        if both == 1:
            sent(1 - upper, g, half)
        else:

            @pl.when(jnp.logical_not(outer))
            def _():
                sent(1 - upper, g, half)

            @pl.when(outer & (lax.rem(g, both) == 0))
            def _():
                sent(1 - upper, g, half, both)

        return c

    def await_unit(source, m, g):
        def await_one(s, c):
            slot_in = m * PER_FRAME + s
            origin = f * span + slot_in
            away = (source != f) | (origin != t)
            two = paired(origin, t)

            @pl.when(away & jnp.logical_not(two))
            def _():
                landed(source, slot_in, g).wait_recv()

            if both > 1:

                @pl.when(away & two & (lax.rem(g, both) == 0))
                def _():
                    landed(source, slot_in, lax.div(g, both) * both, both).wait_recv()

            return c

        with jax.named_scope("await"):
            lax.fori_loop(0, PER_FRAME, await_one, 0)

    def unit(i, c):
        n = lax.div(i, n_fq)
        source = lax.rem(f + lax.rem(i, n_fq), n_fq)
        late = n - (turns - groups)
        first = n < ready
        last = (late >= ready) & (late >= 0)
        inward = first | last
        g = jnp.where(first, n, jnp.where(last, late, lax.rem(n - ready, groups)))
        m = jnp.where(inward, 0, 1 + lax.div(n - ready, groups))
        m = lax.rem(m + inner_frame(f, frames), frames)

        await_unit(source, m, g)
        transform(
            recv.at[source], m, g, chunk, tc, ts, hi, lhs,
            flat.at[:, source * groups + g], m * FFT_LO, frames * FFT_LO,
        )
        return c

    lax.fori_loop(0, (turns - 1) * n_fq, unit, 0)

    def await_last(i, c):
        await_unit(lax.rem(f + i, n_fq), inner_frame(f, frames), groups - 1)
        return c

    lax.fori_loop(0, n_fq, await_last, 0)
    with jax.named_scope("sent"):
        lax.fori_loop(0, groups, all_sent, 0)
        halo_copy(0, right).wait_send()
        halo_copy(1, left).wait_send()


def inner_frame(f, frames):
    return lax.rem(frames - 1 + f, frames)


def last_kernel(n_fq, y, recv, tc, ts, hi, out, tail, lhs, sems, tail_sems):
    f = lax.axis_index("freq")
    parts, blocks, chunk, frames = y.shape[:4]
    groups = blocks // n_fq
    mine = inner_frame(f, frames)
    copies = []
    for p in range(parts):
        for b in range(blocks):
            if b % groups < groups - 1:
                copies.append((y.at[p, b], out.at[p, b]))
            else:
                for j in range(1, frames):
                    m = lax.rem(mine + j, frames)
                    copies.append((y.at[p, b, :, m], out.at[p, b, :, m]))
    copies = [pltpu.make_async_copy(a, b, sems.at[i]) for i, (a, b) in enumerate(copies)]
    for c in copies:
        c.start()

    def tail_copy(p, source):
        return pltpu.make_async_copy(
            tail.at[source, p], out.at[p, source * groups + groups - 1, :, mine], tail_sems.at[p, source]
        )

    def unit(source, c):
        flat = tail.reshape(n_fq, parts, chunk * FFT_LO, FFT_HI)
        transform(
            recv.at[source], mine, groups - 1, chunk, tc, ts, hi, lhs, flat.at[source], 0, FFT_LO
        )
        for p in range(parts):
            tail_copy(p, source).start()
        return c

    lax.fori_loop(0, n_fq, unit, 0)
    for c in copies:
        c.wait()
    for source in range(n_fq):
        for p in range(parts):
            tail_copy(p, source).wait()


def shards(strengths, sample_cell, sample_frac):
    n_tm, n_fq = lax.axis_size("tm"), lax.axis_size("freq")
    parts, groups, channels, samples = strengths.shape
    span = n_tm // n_fq
    frames = span // PER_FRAME
    chunk = channels // n_tm
    rows = parts * chunk
    total = groups * n_tm * rows
    low = np.arange(FFT_LO)[:, None] * np.arange(FFT_HI)[None, :] * (2 * math.pi / FFTLEN)
    high = np.arange(FFT_HI)[:, None] * np.arange(FFT_HI)[None, :] % FFT_HI * (2 * math.pi / FFT_HI)
    hc, hs = np.cos(high), np.sin(high)
    full = np.block([[hc, -hs], [hs, hc]]).astype(np.float32) / math.sqrt(FFTLEN)
    vmem = pl.BlockSpec(memory_space=pltpu.VMEM)
    y_shape = (parts, n_fq * groups, chunk, frames, FFT_LO, FFT_HI)
    results = pl.pallas_call(
        functools.partial(main_kernel, n_tm, n_fq),
        out_shape=(
            pltpu.VMEM(y_shape, jnp.float32),
            pltpu.VMEM((n_fq, span, groups, SLABS, rows, LANES), jnp.bfloat16),
            pltpu.VMEM((FFT_LO, FFT_HI), jnp.float32),
            pltpu.VMEM((FFT_LO, FFT_HI), jnp.float32),
            pltpu.VMEM((2 * FFT_HI, 2 * FFT_HI), jnp.bfloat16),
        ),
        in_specs=[pl.BlockSpec(memory_space=pltpu.HBM)] * 6,
        out_specs=(vmem,) * 5,
        scratch_shapes=[
            pltpu.VMEM((parts, groups, channels, samples), jnp.bfloat16),
            pltpu.VMEM((samples // LANES, LANES), jnp.int32),
            pltpu.VMEM((samples // LANES, LANES), jnp.float32),
            pltpu.VMEM((samples, LANES), jnp.float32),
            pltpu.VMEM((samples, LANES), jnp.float32),
            pltpu.VMEM((samples, (SLABS + 1) * LANES), jnp.bfloat16),
            pltpu.VMEM((2, parts * HALF, total // parts), jnp.float32),
            pltpu.VMEM((2, parts * HALF, total // parts), jnp.float32),
            pltpu.VMEM((n_tm, groups, SLABS, rows, LANES), jnp.bfloat16),
            pltpu.VMEM((FFT_LO * chunk, 2 * FFT_HI), jnp.bfloat16),
            pltpu.SemaphoreType.DMA((5,)),
            pltpu.SemaphoreType.DMA((2 * groups,)),
            pltpu.SemaphoreType.DMA((2, groups)),
            pltpu.SemaphoreType.DMA((n_fq, span, groups)),
            pltpu.SemaphoreType.DMA((2,)),
            pltpu.SemaphoreType.DMA((2,)),
            pltpu.SemaphoreType.REGULAR,
        ],
        compiler_params=pltpu.CompilerParams(
            collective_id=0, has_side_effects=True, vmem_limit_bytes=48 * 1024 * 1024
        ),
        name="grid_exchange_transform",
    )(
        strengths,
        sample_cell.reshape(samples // LANES, LANES),
        sample_frac.reshape(samples // LANES, LANES),
        jnp.asarray(np.cos(low), jnp.float32),
        jnp.asarray(np.sin(low), jnp.float32),
        jnp.asarray(full.astype(jnp.bfloat16)),
    )
    return pl.pallas_call(
        functools.partial(last_kernel, n_fq),
        out_shape=jax.ShapeDtypeStruct(y_shape, jnp.float32),
        in_specs=[vmem] * 5,
        out_specs=pl.BlockSpec(memory_space=pl.ANY),
        scratch_shapes=[
            pltpu.VMEM((n_fq, parts, chunk, FFT_LO, FFT_HI), jnp.float32),
            pltpu.VMEM((FFT_LO * chunk, 2 * FFT_HI), jnp.bfloat16),
            pltpu.SemaphoreType.DMA((parts * n_fq * groups * frames,)),
            pltpu.SemaphoreType.DMA((parts, n_fq)),
        ],
        compiler_params=pltpu.CompilerParams(vmem_limit_bytes=16 * 1024 * 1024),
        name="last_units_write",
    )(*results)


def solution(mesh):
    placed = (P(None, "freq", None, "tm"), P("tm"), P("tm"))
    return jax.shard_map(
        shards,
        mesh=mesh,
        in_specs=placed,
        out_specs=P(None, None, "tm", "freq", None, None),
        check_vma=False,
    )
```

```python
import functools
import math

import jax
import jax.numpy as jnp
import numpy as np
from jax import lax
from jax.experimental import pallas as pl
from jax.experimental.pallas import tpu as pltpu
from jax.sharding import PartitionSpec as P

TAPS = 8
HALF = TAPS // 2
GRID_DEV = 1024
FFT_LO = 32
FFT_HI = 128
FFTLEN = 4096
SHARP = 0.3
MESH = pl.DeviceIdType.MESH
LANES = 128
SLABS = GRID_DEV // LANES
INNER = SLABS - 2
PER_FRAME = FFTLEN // GRID_DEV
EARLY = 3
FIRST = ((0, 2), (2, 2), (4, 2))
PLACE = [INNER] + list(range(INNER)) + [INNER + 1]


def fft_list(re, im):
    n = len(re)
    if n == 1:
        return re, im
    er, ei = fft_list(re[0::2], im[0::2])
    orr, oi = fft_list(re[1::2], im[1::2])
    out_r, out_i = [None] * n, [None] * n
    for k in range(n // 2):
        c, s = math.cos(2 * math.pi * k / n), math.sin(2 * math.pi * k / n)
        a, b = orr[k], oi[k]
        if k == 0:
            tr, ti = a, b
        elif 4 * k == n:
            tr, ti = b, -a
        elif 8 * k == n:
            tr, ti = (a + b) * c, (b - a) * c
        elif 8 * k == 3 * n:
            tr, ti = (b - a) * s, -(a + b) * s
        else:
            tr, ti = a * c + b * s, b * c - a * s
        out_r[k], out_i[k] = er[k] + tr, ei[k] + ti
        out_r[k + n // 2], out_i[k + n // 2] = er[k] - tr, ei[k] - ti
    return out_r, out_i


def sequence(pairs):
    return [(far, pair, core) for pair in reversed(range(pairs)) for core in range(2) for far in (1, 0)]


def transform(blocks, m, g, chunk, tc, ts, hi, lhs, out, start, stride):
    re, im = [], []
    for n in range(FFT_LO):
        tile = blocks[m * PER_FRAME + n // SLABS, g, PLACE[n % SLABS]]
        re.append(tile[:chunk].astype(jnp.float32))
        im.append(tile[chunk:].astype(jnp.float32))
    re, im = fft_list(re, im)
    for a in range(FFT_LO):
        cc = tc[a : a + 1, :]
        ss = ts[a : a + 1, :]
        at = pl.ds(a * chunk, chunk)
        lhs[at, :FFT_HI] = (re[a] * cc + im[a] * ss).astype(jnp.bfloat16)
        lhs[at, FFT_HI:] = (im[a] * cc - re[a] * ss).astype(jnp.bfloat16)
    y = jnp.dot(lhs[...], hi[...], preferred_element_type=jnp.float32)
    for a in range(FFT_LO):
        for p in range(2):
            out[p, pl.ds(start + a, chunk, stride=stride), :] = y[
                a * chunk : (a + 1) * chunk, p * FFT_HI : (p + 1) * FFT_HI
            ]


def main_kernel(
    n_tm, n_fq, strengths, cell_hbm, frac_hbm, tc_hbm, ts_hbm, hi_hbm, y, recv, tc, ts, hi,
    xv, cell, frac, cols, fracs, table, edge_out, halo, src, lhs,
    small, load, send, arrive, halo_send, halo_arrive, ready,
):
    t = lax.axis_index("tm")
    f = lax.axis_index("freq")
    parts, groups, channels, samples = xv.shape
    chunk = channels // n_tm
    rows = src.shape[3]
    wide = channels // 2
    both = groups
    span = n_tm // n_fq
    frames = span // PER_FRAME
    slot = lax.rem(t, span)
    home = lax.div(t, span)
    half = n_tm // 2
    block = half * rows
    upper = lax.div(t, half)
    quarter = lax.div(t, n_tm // 4)
    outer = (quarter == 0) | (quarter == 3)
    right = lax.rem(t + 1, n_tm)
    left = lax.rem(t + n_tm - 1, n_tm)
    steps = 2 * groups
    early = min(EARLY, steps)
    keep = home == f

    def order(k):
        ahead = (k == 0) | ((lax.rem(k, 2) == 1) & (k < steps - 1))
        far = jnp.where(outer, k >= groups, ahead)
        inward = jnp.where(ahead, lax.div(k + 1, 2), lax.div(k - 1, 2))
        side = jnp.where(far, 1 - upper, upper)
        return side, jnp.where(outer, lax.rem(k, groups), inward)

    constants = [
        pltpu.make_async_copy(a, b, small.at[i])
        for i, (a, b) in enumerate(
            ((cell_hbm, cell), (frac_hbm, frac), (tc_hbm, tc), (ts_hbm, ts), (hi_hbm, hi))
        )
    ]
    for i in range(2):
        constants[i].start()

    barrier = pltpu.get_barrier_semaphore()
    size = n_tm // 4
    mate = jnp.where((quarter == 0) | (quarter == 2), t + size, t - size)

    def outer_of(index):
        q = lax.div(index, size)
        return jnp.where(q == 1, index - size, jnp.where(q == 2, index + size, index))

    def greet_one(tm, freq):
        pl.semaphore_signal(barrier, inc=1, device_id=(tm, freq), device_id_type=MESH)

    def greet(i, c):
        origin = f * span + lax.rem(slot + 1 + i, span)
        host = outer_of(origin)
        facing = jnp.logical_not(outer) & (lax.div(origin, size) == 3 - quarter)

        def one(j, c):
            other = lax.rem(f + j, n_fq)

            @pl.when(facing)
            def _():
                greet_one(origin, other)

            @pl.when((host != t) | (other != f))
            def _():
                greet_one(host, other)

            return c

        return lax.fori_loop(0, n_fq, one, c)

    lax.fori_loop(0, span, greet, 0)
    greet_one(outer_of(left), f)
    greet_one(outer_of(right), f)

    @pl.when(jnp.logical_not(outer))
    def _():
        greet_one(mate, f)

    def greeted():
        own = jnp.where(keep, n_tm - 1, n_tm)
        others = jnp.where(lax.div(mate, span) == f, n_tm - 1, n_tm)
        pl.semaphore_wait(barrier, jnp.where(outer, own + others + 5, size))

        @pl.when(outer)
        def _():
            pl.semaphore_signal(ready, inc=1, device_id=(mate, f), device_id_type=MESH)

    def fetch(i):
        if i == 2:
            at = (slice(None), pl.ds(1, groups - 1))
        else:
            side = order(0)[0]
            side = side if i == 0 else 1 - side
            at = (slice(None), 0, pl.ds(pl.multiple_of(side * wide, wide), wide))
        return pltpu.make_async_copy(strengths.at[at], xv.at[at], load.at[i])

    fetches = 3 if groups > 1 else 2
    fetch(0).start()

    for i in range(1, fetches):
        fetch(i).start()

    base = t * GRID_DEV
    constants[0].wait()
    constants[1].wait()
    for i in range(samples // LANES):
        at = pl.ds(i * LANES, LANES)
        local = (cell[i : i + 1, :] - base).astype(jnp.float32)
        cols[at, :] = jnp.broadcast_to(local, (LANES, LANES)).T
        fracs[at, :] = jnp.broadcast_to(frac[i : i + 1, :], (LANES, LANES)).T
    lane = lax.broadcasted_iota(jnp.int32, (LANES, LANES), 1)

    def build(place, columns):
        def part(i, c):
            at = pl.ds(pl.multiple_of(i * LANES, LANES), LANES)
            d = columns - cols[at, :]
            u = d - fracs[at, :]
            w = jnp.exp(-SHARP * (u * u))
            inside = jnp.abs(d - 0.5) < float(HALF)
            table[at, place * LANES : (place + 1) * LANES] = jnp.where(inside, w, 0.0).astype(jnp.bfloat16)
            return c

        lax.fori_loop(0, samples // LANES, part, 0, unroll=4)

    def slab_columns(j):
        return (lane + j * LANES).astype(jnp.float32)

    def operand(k):
        side, g = order(k)
        at = pl.ds(pl.multiple_of(side * wide, wide), wide)
        return xv[:, g, at, :].reshape(block, samples)

    def product(k, first, count):
        return jnp.dot(
            operand(k),
            table[:, first * LANES : (first + count) * LANES],
            preferred_element_type=jnp.float32,
        )

    def put(k, first, pieces):
        side, g = order(k)
        for j, part in enumerate(pieces):
            part = part.astype(jnp.bfloat16)
            for i in range(half):
                for p in range(parts):
                    start = p * wide + i * chunk
                    src[side * half + i, g, first + j, p * chunk : (p + 1) * chunk] = part[start : start + chunk]

    def slabs(acc):
        return [acc[:, j : j + LANES] for j in range(0, acc.shape[1], LANES)]

    def with_halo(k, low, high):
        side, g = order(k)
        at = pl.ds(pl.multiple_of(g * channels + side * wide, LANES), wide)
        empty = jnp.zeros((LANES - 2 * HALF, wide), jnp.float32)
        outside = jnp.concatenate(
            [
                jnp.concatenate(
                    [halo[0, p * HALF : (p + 1) * HALF, at], empty, halo[1, p * HALF : (p + 1) * HALF, at]]
                ).T
                for p in range(parts)
            ]
        )
        spot = lax.broadcasted_iota(jnp.int32, (block, LANES), 1)
        return [
            low + jnp.where(spot < LANES // 2, outside, 0.0),
            high + jnp.where(spot >= LANES // 2, outside, 0.0),
        ]

    def copy_out(d, g, first, count, pair=1):
        part = (pl.ds(g, pair), pl.ds(first, count))
        return pltpu.make_async_remote_copy(
            src_ref=src.at[(d,) + part],
            dst_ref=recv.at[(f, slot) + part],
            send_sem=send.at[lax.div(d, half)],
            recv_sem=arrive.at[f, lax.div(slot, PER_FRAME), g],
            device_id=(d, home),
            device_id_type=MESH,
        )

    pairs = n_tm // 8
    pair_at = lax.rem(lax.div(t, 2), pairs)
    core_at = lax.rem(t, 2)

    def target(side, far, pair, core):
        across = lax.rem(side + 1 + far, 2)
        return side * half + across * (half // 2) + lax.rem(pair_at + pair, pairs) * 2 + lax.rem(core_at + core, 2)


    def send_step(k, first, count, pair=1, which=(0, 1)):
        side, g = order(k)
        for far, pair_by, core_by in sequence(pairs):
            if far not in which:
                continue
            d = target(side, far, pair_by, core_by)

            @pl.when((d != t) | (home != f))
            def _():
                copy_out(d, g - (pair - 1), first, count, pair).start()

    fetch(0).wait()
    with jax.named_scope("first"):
        for first, count in FIRST:
            for j in range(first, first + count):
                build(j, slab_columns(1 + j))
            put(0, first, slabs(product(0, first, count)))
            if first == 0:
                with jax.named_scope("bar"):
                    greeted()
            send_step(0, first, count, which=(0,))
            if first == 0:
                for i in range(2, 5):
                    constants[i].start()

        with jax.named_scope("ready"):

            @pl.when(jnp.logical_not(outer))
            def _():
                pl.semaphore_wait(ready, 1)

        send_step(0, 0, INNER, which=(1,))

    beyond = jnp.where(
        lane < HALF, lane + GRID_DEV, jnp.where(lane < 2 * HALF, lane - 2 * HALF, -GRID_DEV)
    ).astype(jnp.float32)

    def edges(g, c):
        acc = jnp.dot(
            xv[:, g].reshape(2 * block, samples),
            table[:, SLABS * LANES :],
            preferred_element_type=jnp.float32,
        )
        across = acc.T[: 2 * HALF]
        at = pl.ds(pl.multiple_of(g * channels, LANES), channels)
        for side in range(2):
            edge_out[side, :, at] = jnp.concatenate(
                [
                    across[side * HALF : (side + 1) * HALF, p * channels : (p + 1) * channels]
                    for p in range(parts)
                ]
            )
        return c

    with jax.named_scope("edges"):
        build(SLABS, beyond)
        for i in range(1, fetches):
            fetch(i).wait()
        lax.fori_loop(0, groups, edges, 0)

    def halo_copy(i, peer):
        return pltpu.make_async_remote_copy(
            src_ref=edge_out.at[i],
            dst_ref=halo.at[i],
            send_sem=halo_send.at[i],
            recv_sem=halo_arrive.at[i],
            device_id=(peer, f),
            device_id_type=MESH,
        )

    halo_copy(0, right).start()
    halo_copy(1, left).start()

    def early_step(k, c):
        put(k, 0, slabs(product(k, 0, INNER)))
        send_step(k, 0, INNER)
        return c

    with jax.named_scope("early"):
        lax.fori_loop(1, early, early_step, 0)
        build(INNER, slab_columns(0))
        build(INNER + 1, slab_columns(SLABS - 1))
    with jax.named_scope("halo_wait"):
        halo_copy(0, right).wait_recv()
        halo_copy(1, left).wait_recv()

    def early_edges(k, c):
        put(k, INNER, with_halo(k, *slabs(product(k, INNER, 2))))
        send_step(k, INNER, 2)
        return c

    def late_step(k, c):
        pieces = slabs(product(k, 0, SLABS))
        put(k, 0, pieces[:INNER] + with_halo(k, *pieces[INNER:]))
        if both == 1:
            send_step(k, 0, SLABS)
        else:
            in_pairs = outer & (k >= groups)

            @pl.when(in_pairs & (lax.rem(k, both) == both - 1))
            def _():
                send_step(k, 0, SLABS, both)

            @pl.when(jnp.logical_not(in_pairs))
            def _():
                send_step(k, 0, SLABS)

        return c

    with jax.named_scope("early_edges"):
        lax.fori_loop(0, early, early_edges, 0)
    with jax.named_scope("late"):
        lax.fori_loop(early, steps, late_step, 0)

    @pl.when(keep)
    def _():
        def own(g, c):
            recv[f, slot, g] = src[t, g]
            return c

        lax.fori_loop(0, groups, own, 0)

    def landed(source, m, g, pair=1, count=PER_FRAME):
        part = recv.at[source, pl.ds(m * PER_FRAME, count), pl.ds(g, pair)]
        return pltpu.make_async_remote_copy(
            src_ref=part,
            dst_ref=part,
            send_sem=send.at[0],
            recv_sem=arrive.at[source, m, g],
            device_id=(t, f),
            device_id_type=MESH,
        )

    def is_outer(index):
        q = lax.div(index, n_tm // 4)
        return (q == 0) | (q == 3)

    def paired(origin, d):
        return is_outer(origin) & (lax.div(origin, half) != lax.div(d, half)) & (both > 1)

    for i in range(2, 5):
        constants[i].wait()
    flat = y.reshape(2, n_fq * groups, chunk * frames * FFT_LO, FFT_HI)
    ready = min(2, groups)
    turns = frames * groups

    def sent(side, count):
        part = src.at[pl.ds(side * half, count)]
        pltpu.make_async_remote_copy(
            src_ref=part,
            dst_ref=part,
            send_sem=send.at[side],
            recv_sem=arrive.at[0, 0, 0],
            device_id=(right, f),
            device_id_type=MESH,
        ).wait_send()

    def all_sent():
        @pl.when(keep)
        def _():
            sent(upper, half - 1)

        @pl.when(jnp.logical_not(keep))
        def _():
            sent(upper, half)

        sent(1 - upper, half)

    def await_unit(source, m, g):
        origin = f * span + m * PER_FRAME
        own = (source == f) & (lax.div(t, PER_FRAME) == lax.div(origin, PER_FRAME))
        two = paired(origin, t)
        with jax.named_scope("await"):

            @pl.when(own)
            def _():
                landed(source, m, g, count=PER_FRAME - 1).wait_recv()

            @pl.when(jnp.logical_not(own | two))
            def _():
                landed(source, m, g).wait_recv()

            if both > 1:

                @pl.when(two & (lax.rem(g, both) == 0))
                def _():
                    landed(source, m, lax.div(g, both) * both, both).wait_recv()

    def unit(i, c):
        n = lax.div(i, n_fq)
        source = lax.rem(f + lax.rem(i, n_fq), n_fq)
        late = n - (turns - groups)
        first = n < ready
        last = (late >= ready) & (late >= 0)
        inward = first | last
        g = jnp.where(first, n, jnp.where(last, late, lax.rem(n - ready, groups)))
        m = jnp.where(inward, 0, 1 + lax.div(n - ready, groups))
        m = lax.rem(m + inner_frame(f, frames), frames)

        await_unit(source, m, g)
        transform(
            recv.at[source], m, g, chunk, tc, ts, hi, lhs,
            flat.at[:, source * groups + g], m * FFT_LO, frames * FFT_LO,
        )
        return c

    lax.fori_loop(0, (turns - 1) * n_fq, unit, 0)

    def await_last(i, c):
        await_unit(lax.rem(f + i, n_fq), inner_frame(f, frames), groups - 1)
        return c

    lax.fori_loop(0, n_fq, await_last, 0)
    with jax.named_scope("sent"):
        all_sent()
        halo_copy(0, right).wait_send()
        halo_copy(1, left).wait_send()


def inner_frame(f, frames):
    return lax.rem(frames - 1 + f, frames)


def last_kernel(n_fq, y, recv, tc, ts, hi, out, tail, lhs, sems):
    f = lax.axis_index("freq")
    parts, blocks, chunk, frames = y.shape[:4]
    groups = blocks // n_fq
    mine = inner_frame(f, frames)
    def copy(a, b, i):
        return pltpu.make_async_copy(a, b, sems.at[i])

    for p in range(parts):
        for b in range(blocks):
            if b % groups < groups - 1:
                copy(y.at[p, b], out.at[p, b], 0).start()
            else:
                for j in range(1, frames):
                    m = lax.rem(mine + j, frames)
                    copy(y.at[p, b, :, m], out.at[p, b, :, m], 1).start()

    def unit(source, c):
        flat = tail.reshape(parts, n_fq, chunk * FFT_LO, FFT_HI)
        transform(
            recv.at[source], mine, groups - 1, chunk, tc, ts, hi, lhs, flat.at[:, source], 0, FFT_LO
        )
        for p in range(parts):
            copy(tail.at[p, source], out.at[p, source * groups + groups - 1, :, mine], 2).start()
        return c

    lax.fori_loop(0, n_fq, unit, 0)
    if groups > 1:
        at = (slice(None), pl.ds(0, n_fq * (groups - 1)))
        copy(y.at[at], out.at[at], 0).wait()
    if frames > 1:
        at = (slice(None), pl.ds(0, n_fq), slice(None), pl.ds(0, frames - 1))
        copy(y.at[at], out.at[at], 1).wait()
    copy(tail, out.at[:, pl.ds(0, n_fq), :, 0], 2).wait()


def shards(strengths, sample_cell, sample_frac):
    n_tm, n_fq = lax.axis_size("tm"), lax.axis_size("freq")
    parts, groups, channels, samples = strengths.shape
    span = n_tm // n_fq
    frames = span // PER_FRAME
    chunk = channels // n_tm
    rows = parts * chunk
    total = groups * n_tm * rows
    low = np.arange(FFT_LO)[:, None] * np.arange(FFT_HI)[None, :] * (2 * math.pi / FFTLEN)
    high = np.arange(FFT_HI)[:, None] * np.arange(FFT_HI)[None, :] % FFT_HI * (2 * math.pi / FFT_HI)
    hc, hs = np.cos(high), np.sin(high)
    full = np.block([[hc, -hs], [hs, hc]]).astype(np.float32) / math.sqrt(FFTLEN)
    vmem = pl.BlockSpec(memory_space=pltpu.VMEM)
    y_shape = (parts, n_fq * groups, chunk, frames, FFT_LO, FFT_HI)
    results = pl.pallas_call(
        functools.partial(main_kernel, n_tm, n_fq),
        out_shape=(
            pltpu.VMEM(y_shape, jnp.float32),
            pltpu.VMEM((n_fq, span, groups, SLABS, rows, LANES), jnp.bfloat16),
            pltpu.VMEM((FFT_LO, FFT_HI), jnp.float32),
            pltpu.VMEM((FFT_LO, FFT_HI), jnp.float32),
            pltpu.VMEM((2 * FFT_HI, 2 * FFT_HI), jnp.bfloat16),
        ),
        in_specs=[pl.BlockSpec(memory_space=pltpu.HBM)] * 6,
        out_specs=(vmem,) * 5,
        scratch_shapes=[
            pltpu.VMEM((parts, groups, channels, samples), jnp.bfloat16),
            pltpu.VMEM((samples // LANES, LANES), jnp.int32),
            pltpu.VMEM((samples // LANES, LANES), jnp.float32),
            pltpu.VMEM((samples, LANES), jnp.float32),
            pltpu.VMEM((samples, LANES), jnp.float32),
            pltpu.VMEM((samples, (SLABS + 1) * LANES), jnp.bfloat16),
            pltpu.VMEM((2, parts * HALF, total // parts), jnp.float32),
            pltpu.VMEM((2, parts * HALF, total // parts), jnp.float32),
            pltpu.VMEM((n_tm, groups, SLABS, rows, LANES), jnp.bfloat16),
            pltpu.VMEM((FFT_LO * chunk, 2 * FFT_HI), jnp.bfloat16),
            pltpu.SemaphoreType.DMA((5,)),
            pltpu.SemaphoreType.DMA((3,)),
            pltpu.SemaphoreType.DMA((2,)),
            pltpu.SemaphoreType.DMA((n_fq, frames, groups)),
            pltpu.SemaphoreType.DMA((2,)),
            pltpu.SemaphoreType.DMA((2,)),
            pltpu.SemaphoreType.REGULAR,
        ],
        compiler_params=pltpu.CompilerParams(
            collective_id=0, has_side_effects=True, vmem_limit_bytes=48 * 1024 * 1024
        ),
        name="grid_exchange_transform",
    )(
        strengths,
        sample_cell.reshape(samples // LANES, LANES),
        sample_frac.reshape(samples // LANES, LANES),
        jnp.asarray(np.cos(low), jnp.float32),
        jnp.asarray(np.sin(low), jnp.float32),
        jnp.asarray(full.astype(jnp.bfloat16)),
    )
    return pl.pallas_call(
        functools.partial(last_kernel, n_fq),
        out_shape=jax.ShapeDtypeStruct(y_shape, jnp.float32),
        in_specs=[vmem] * 5,
        out_specs=pl.BlockSpec(memory_space=pl.ANY),
        scratch_shapes=[
            pltpu.VMEM((parts, n_fq, chunk, FFT_LO, FFT_HI), jnp.float32),
            pltpu.VMEM((FFT_LO * chunk, 2 * FFT_HI), jnp.bfloat16),
            pltpu.SemaphoreType.DMA((3,)),
        ],
        compiler_params=pltpu.CompilerParams(vmem_limit_bytes=16 * 1024 * 1024),
        name="last_units_write",
    )(*results)


def solution(mesh):
    placed = (P(None, "freq", None, "tm"), P("tm"), P("tm"))
    return jax.shard_map(
        shards,
        mesh=mesh,
        in_specs=placed,
        out_specs=P(None, None, "tm", "freq", None, None),
        check_vma=False,
    )
```

```python
import functools
import math

import jax
import jax.numpy as jnp
import numpy as np
from jax import lax
from jax.experimental import pallas as pl
from jax.experimental.pallas import tpu as pltpu
from jax.sharding import PartitionSpec as P

TAPS = 8
HALF = TAPS // 2
GRID_DEV = 1024
FFT_LO = 32
FFT_HI = 128
FFTLEN = 4096
SHARP = 0.3
MESH = pl.DeviceIdType.MESH
LANES = 128
SLABS = GRID_DEV // LANES
INNER = SLABS - 2
PER_FRAME = FFTLEN // GRID_DEV
EARLY = 2
FIRST = ((0, 2), (2, 2), (4, 2))
PLACE = [INNER] + list(range(INNER)) + [INNER + 1]


def fft_list(re, im):
    n = len(re)
    if n == 1:
        return re, im
    er, ei = fft_list(re[0::2], im[0::2])
    orr, oi = fft_list(re[1::2], im[1::2])
    out_r, out_i = [None] * n, [None] * n
    for k in range(n // 2):
        c, s = math.cos(2 * math.pi * k / n), math.sin(2 * math.pi * k / n)
        a, b = orr[k], oi[k]
        if k == 0:
            tr, ti = a, b
        elif 4 * k == n:
            tr, ti = b, -a
        elif 8 * k == n:
            tr, ti = (a + b) * c, (b - a) * c
        elif 8 * k == 3 * n:
            tr, ti = (b - a) * s, -(a + b) * s
        else:
            tr, ti = a * c + b * s, b * c - a * s
        out_r[k], out_i[k] = er[k] + tr, ei[k] + ti
        out_r[k + n // 2], out_i[k + n // 2] = er[k] - tr, ei[k] - ti
    return out_r, out_i


def sequence(pairs):
    return [(far, pair, core) for pair in reversed(range(pairs)) for core in range(2) for far in (1, 0)]


def transform(blocks, m, g, chunk, tc, ts, hi, lhs, out, start, stride):
    re, im = [], []
    for n in range(FFT_LO):
        tile = blocks[m * PER_FRAME + n // SLABS, g, PLACE[n % SLABS]]
        re.append(tile[:chunk].astype(jnp.float32))
        im.append(tile[chunk:].astype(jnp.float32))
    re, im = fft_list(re, im)
    for a in range(FFT_LO):
        cc = tc[a : a + 1, :]
        ss = ts[a : a + 1, :]
        at = pl.ds(a * chunk, chunk)
        lhs[at, :FFT_HI] = (re[a] * cc + im[a] * ss).astype(jnp.bfloat16)
        lhs[at, FFT_HI:] = (im[a] * cc - re[a] * ss).astype(jnp.bfloat16)
    y = jnp.dot(lhs[...], hi[...], preferred_element_type=jnp.float32)
    for a in range(FFT_LO):
        for p in range(2):
            out[p, pl.ds(start + a, chunk, stride=stride), :] = y[
                a * chunk : (a + 1) * chunk, p * FFT_HI : (p + 1) * FFT_HI
            ]


def main_kernel(
    n_tm, n_fq, strengths, cell_hbm, frac_hbm, tc_hbm, ts_hbm, hi_hbm, y, recv, tc, ts, hi,
    xv, cell, frac, cols, fracs, table, edge_out, halo, src, lhs,
    small, load, send, arrive, halo_send, halo_arrive, ready,
):
    t = lax.axis_index("tm")
    f = lax.axis_index("freq")
    parts, groups, channels, samples = xv.shape
    chunk = channels // n_tm
    rows = src.shape[3]
    wide = channels // 2
    both = groups
    span = n_tm // n_fq
    frames = span // PER_FRAME
    slot = lax.rem(t, span)
    home = lax.div(t, span)
    half = n_tm // 2
    block = half * rows
    upper = lax.div(t, half)
    quarter = lax.div(t, n_tm // 4)
    outer = (quarter == 0) | (quarter == 3)
    right = lax.rem(t + 1, n_tm)
    left = lax.rem(t + n_tm - 1, n_tm)
    steps = 2 * groups
    early = min(EARLY, steps)
    keep = home == f

    def order(k):
        ahead = (k == 0) | ((lax.rem(k, 2) == 1) & (k < steps - 1))
        far = jnp.where(outer, k >= groups, ahead)
        inward = jnp.where(ahead, lax.div(k + 1, 2), lax.div(k - 1, 2))
        side = jnp.where(far, 1 - upper, upper)
        return side, jnp.where(outer, lax.rem(k, groups), inward)

    constants = [
        pltpu.make_async_copy(a, b, small.at[i])
        for i, (a, b) in enumerate(
            ((cell_hbm, cell), (frac_hbm, frac), (tc_hbm, tc), (ts_hbm, ts), (hi_hbm, hi))
        )
    ]
    for i in range(2):
        constants[i].start()

    barrier = pltpu.get_barrier_semaphore()
    size = n_tm // 4
    mate = jnp.where((quarter == 0) | (quarter == 2), t + size, t - size)

    def outer_of(index):
        q = lax.div(index, size)
        return jnp.where(q == 1, index - size, jnp.where(q == 2, index + size, index))

    def greet_one(tm, freq):
        pl.semaphore_signal(barrier, inc=1, device_id=(tm, freq), device_id_type=MESH)

    def greet(i, c):
        origin = f * span + lax.rem(slot + 1 + i, span)
        host = outer_of(origin)
        facing = jnp.logical_not(outer) & (lax.div(origin, size) == 3 - quarter)

        def one(j, c):
            other = lax.rem(f + j, n_fq)

            @pl.when(facing)
            def _():
                greet_one(origin, other)

            @pl.when((host != t) | (other != f))
            def _():
                greet_one(host, other)

            return c

        return lax.fori_loop(0, n_fq, one, c)

    lax.fori_loop(0, span, greet, 0)
    greet_one(outer_of(left), f)
    greet_one(outer_of(right), f)

    @pl.when(jnp.logical_not(outer))
    def _():
        greet_one(mate, f)

    def greeted():
        own = jnp.where(keep, n_tm - 1, n_tm)
        others = jnp.where(lax.div(mate, span) == f, n_tm - 1, n_tm)
        pl.semaphore_wait(barrier, jnp.where(outer, own + others + 5, size))

        @pl.when(outer)
        def _():
            pl.semaphore_signal(ready, inc=1, device_id=(mate, f), device_id_type=MESH)

    def fetch(i):
        if i == 2:
            at = (slice(None), pl.ds(1, groups - 1))
        else:
            side = order(0)[0]
            side = side if i == 0 else 1 - side
            at = (slice(None), 0, pl.ds(pl.multiple_of(side * wide, wide), wide))
        return pltpu.make_async_copy(strengths.at[at], xv.at[at], load.at[i])

    fetches = 3 if groups > 1 else 2
    fetch(0).start()

    for i in range(1, fetches):
        fetch(i).start()

    base = t * GRID_DEV
    constants[0].wait()
    constants[1].wait()
    for i in range(samples // LANES):
        at = pl.ds(i * LANES, LANES)
        local = (cell[i : i + 1, :] - base).astype(jnp.float32)
        cols[at, :] = jnp.broadcast_to(local, (LANES, LANES)).T
        fracs[at, :] = jnp.broadcast_to(frac[i : i + 1, :], (LANES, LANES)).T
    lane = lax.broadcasted_iota(jnp.int32, (LANES, LANES), 1)

    def build(place, columns):
        def part(i, c):
            at = pl.ds(pl.multiple_of(i * LANES, LANES), LANES)
            d = columns - cols[at, :]
            u = d - fracs[at, :]
            w = jnp.exp(-SHARP * (u * u))
            inside = jnp.abs(d - 0.5) < float(HALF)
            table[at, place * LANES : (place + 1) * LANES] = jnp.where(inside, w, 0.0).astype(jnp.bfloat16)
            return c

        lax.fori_loop(0, samples // LANES, part, 0, unroll=4)

    def slab_columns(j):
        return (lane + j * LANES).astype(jnp.float32)

    def operand(k):
        side, g = order(k)
        at = pl.ds(pl.multiple_of(side * wide, wide), wide)
        return xv[:, g, at, :].reshape(block, samples)

    def product(k, first, count):
        return jnp.dot(
            operand(k),
            table[:, first * LANES : (first + count) * LANES],
            preferred_element_type=jnp.float32,
        )

    def put(k, first, pieces):
        side, g = order(k)
        for j, part in enumerate(pieces):
            part = part.astype(jnp.bfloat16)
            for i in range(half):
                for p in range(parts):
                    start = p * wide + i * chunk
                    src[side * half + i, g, first + j, p * chunk : (p + 1) * chunk] = part[start : start + chunk]

    def slabs(acc):
        return [acc[:, j : j + LANES] for j in range(0, acc.shape[1], LANES)]

    def with_halo(k, low, high):
        side, g = order(k)
        at = pl.ds(pl.multiple_of(g * channels + side * wide, LANES), wide)
        empty = jnp.zeros((LANES - 2 * HALF, wide), jnp.float32)
        outside = jnp.concatenate(
            [
                jnp.concatenate(
                    [halo[0, p * HALF : (p + 1) * HALF, at], empty, halo[1, p * HALF : (p + 1) * HALF, at]]
                ).T
                for p in range(parts)
            ]
        )
        spot = lax.broadcasted_iota(jnp.int32, (block, LANES), 1)
        return [
            low + jnp.where(spot < LANES // 2, outside, 0.0),
            high + jnp.where(spot >= LANES // 2, outside, 0.0),
        ]

    def copy_out(d, g, first, count, pair=1):
        part = (pl.ds(g, pair), pl.ds(first, count))
        return pltpu.make_async_remote_copy(
            src_ref=src.at[(d,) + part],
            dst_ref=recv.at[(f, slot) + part],
            send_sem=send.at[lax.div(d, half)],
            recv_sem=arrive.at[f, lax.div(slot, PER_FRAME), g],
            device_id=(d, home),
            device_id_type=MESH,
        )

    pairs = n_tm // 8
    pair_at = lax.rem(lax.div(t, 2), pairs)
    core_at = lax.rem(t, 2)

    def target(side, far, pair, core):
        across = lax.rem(side + 1 + far, 2)
        return side * half + across * (half // 2) + lax.rem(pair_at + pair, pairs) * 2 + lax.rem(core_at + core, 2)


    def send_step(k, first, count, pair=1, which=(0, 1)):
        side, g = order(k)
        for far, pair_by, core_by in sequence(pairs):
            if far not in which:
                continue
            d = target(side, far, pair_by, core_by)

            @pl.when((d != t) | (home != f))
            def _():
                copy_out(d, g - (pair - 1), first, count, pair).start()

    fetch(0).wait()
    with jax.named_scope("first"):
        for first, count in FIRST:
            for j in range(first, first + count):
                build(j, slab_columns(1 + j))
            put(0, first, slabs(product(0, first, count)))
            if first == 0:
                with jax.named_scope("bar"):
                    greeted()
            send_step(0, first, count, which=(0,))
            if first == 0:
                for i in range(2, 5):
                    constants[i].start()

        with jax.named_scope("ready"):

            @pl.when(jnp.logical_not(outer))
            def _():
                pl.semaphore_wait(ready, 1)

        send_step(0, 0, INNER, which=(1,))

    beyond = jnp.where(
        lane < HALF, lane + GRID_DEV, jnp.where(lane < 2 * HALF, lane - 2 * HALF, -GRID_DEV)
    ).astype(jnp.float32)

    def edges(g, c):
        acc = jnp.dot(
            xv[:, g].reshape(2 * block, samples),
            table[:, SLABS * LANES :],
            preferred_element_type=jnp.float32,
        )
        across = acc.T[: 2 * HALF]
        at = pl.ds(pl.multiple_of(g * channels, LANES), channels)
        for side in range(2):
            edge_out[side, :, at] = jnp.concatenate(
                [
                    across[side * HALF : (side + 1) * HALF, p * channels : (p + 1) * channels]
                    for p in range(parts)
                ]
            )
        return c

    with jax.named_scope("edges"):
        build(SLABS, beyond)
        for i in range(1, fetches):
            fetch(i).wait()
        lax.fori_loop(0, groups, edges, 0)

    def halo_copy(i, peer):
        return pltpu.make_async_remote_copy(
            src_ref=edge_out.at[i],
            dst_ref=halo.at[i],
            send_sem=halo_send.at[i],
            recv_sem=halo_arrive.at[i],
            device_id=(peer, f),
            device_id_type=MESH,
        )

    halo_copy(0, right).start()
    halo_copy(1, left).start()

    def early_step(k, c):
        put(k, 0, slabs(product(k, 0, INNER)))
        send_step(k, 0, INNER)
        return c

    with jax.named_scope("early"):
        lax.fori_loop(1, early, early_step, 0)
        build(INNER, slab_columns(0))
        build(INNER + 1, slab_columns(SLABS - 1))
    with jax.named_scope("halo_wait"):
        halo_copy(0, right).wait_recv()
        halo_copy(1, left).wait_recv()

    def early_edges(k, c):
        put(k, INNER, with_halo(k, *slabs(product(k, INNER, 2))))
        send_step(k, INNER, 2)
        return c

    def late_step(k, c):
        pieces = slabs(product(k, 0, SLABS))
        put(k, 0, pieces[:INNER] + with_halo(k, *pieces[INNER:]))
        if both == 1:
            send_step(k, 0, SLABS)
        else:
            in_pairs = outer & (k >= groups)

            @pl.when(in_pairs & (lax.rem(k, both) == both - 1))
            def _():
                send_step(k, 0, SLABS, both)

            @pl.when(jnp.logical_not(in_pairs))
            def _():
                send_step(k, 0, SLABS)

        return c

    with jax.named_scope("early_edges"):
        lax.fori_loop(0, early, early_edges, 0)
    with jax.named_scope("late"):
        lax.fori_loop(early, steps, late_step, 0)

    @pl.when(keep)
    def _():
        def own(g, c):
            recv[f, slot, g] = src[t, g]
            return c

        lax.fori_loop(0, groups, own, 0)

    def landed(source, m, g, pair=1, count=PER_FRAME):
        part = recv.at[source, pl.ds(m * PER_FRAME, count), pl.ds(g, pair)]
        return pltpu.make_async_remote_copy(
            src_ref=part,
            dst_ref=part,
            send_sem=send.at[0],
            recv_sem=arrive.at[source, m, g],
            device_id=(t, f),
            device_id_type=MESH,
        )

    def is_outer(index):
        q = lax.div(index, n_tm // 4)
        return (q == 0) | (q == 3)

    def paired(origin, d):
        return is_outer(origin) & (lax.div(origin, half) != lax.div(d, half)) & (both > 1)

    for i in range(2, 5):
        constants[i].wait()
    flat = y.reshape(2, n_fq * groups, chunk * frames * FFT_LO, FFT_HI)
    ready = min(2, groups)
    turns = frames * groups

    def sent(side, count):
        part = src.at[pl.ds(side * half, count)]
        pltpu.make_async_remote_copy(
            src_ref=part,
            dst_ref=part,
            send_sem=send.at[side],
            recv_sem=arrive.at[0, 0, 0],
            device_id=(right, f),
            device_id_type=MESH,
        ).wait_send()

    def all_sent():
        @pl.when(keep)
        def _():
            sent(upper, half - 1)

        @pl.when(jnp.logical_not(keep))
        def _():
            sent(upper, half)

        sent(1 - upper, half)

    def await_unit(source, m, g):
        origin = f * span + m * PER_FRAME
        own = (source == f) & (lax.div(t, PER_FRAME) == lax.div(origin, PER_FRAME))
        two = paired(origin, t)
        with jax.named_scope("await"):

            @pl.when(own)
            def _():
                landed(source, m, g, count=PER_FRAME - 1).wait_recv()

            @pl.when(jnp.logical_not(own | two))
            def _():
                landed(source, m, g).wait_recv()

            if both > 1:

                @pl.when(two & (lax.rem(g, both) == 0))
                def _():
                    landed(source, m, lax.div(g, both) * both, both).wait_recv()

    def unit(i, c):
        n = lax.div(i, n_fq)
        source = lax.rem(f + lax.rem(i, n_fq), n_fq)
        late = n - (turns - groups)
        first = n < ready
        last = (late >= ready) & (late >= 0)
        inward = first | last
        g = jnp.where(first, n, jnp.where(last, late, lax.rem(n - ready, groups)))
        m = jnp.where(inward, 0, 1 + lax.div(n - ready, groups))
        m = lax.rem(m + inner_frame(f, frames), frames)

        await_unit(source, m, g)
        transform(
            recv.at[source], m, g, chunk, tc, ts, hi, lhs,
            flat.at[:, source * groups + g], m * FFT_LO, frames * FFT_LO,
        )
        return c

    lax.fori_loop(0, (turns - 1) * n_fq, unit, 0)

    def await_last(i, c):
        await_unit(lax.rem(f + i, n_fq), inner_frame(f, frames), groups - 1)
        return c

    lax.fori_loop(0, n_fq, await_last, 0)
    with jax.named_scope("sent"):
        all_sent()
        halo_copy(0, right).wait_send()
        halo_copy(1, left).wait_send()


def inner_frame(f, frames):
    return lax.rem(frames - 1 + f, frames)


def last_kernel(n_fq, y, recv, tc, ts, hi, out, tail, lhs, sems):
    f = lax.axis_index("freq")
    parts, blocks, chunk, frames = y.shape[:4]
    groups = blocks // n_fq
    mine = inner_frame(f, frames)
    def copy(a, b, i):
        return pltpu.make_async_copy(a, b, sems.at[i])

    for p in range(parts):
        for b in range(blocks):
            if b % groups < groups - 1:
                copy(y.at[p, b], out.at[p, b], 0).start()
            else:
                for j in range(1, frames):
                    m = lax.rem(mine + j, frames)
                    copy(y.at[p, b, :, m], out.at[p, b, :, m], 1).start()

    def unit(source, c):
        flat = tail.reshape(parts, n_fq, chunk * FFT_LO, FFT_HI)
        transform(
            recv.at[source], mine, groups - 1, chunk, tc, ts, hi, lhs, flat.at[:, source], 0, FFT_LO
        )
        for p in range(parts):
            copy(tail.at[p, source], out.at[p, source * groups + groups - 1, :, mine], 2).start()
        return c

    lax.fori_loop(0, n_fq, unit, 0)
    if groups > 1:
        at = (slice(None), pl.ds(0, n_fq * (groups - 1)))
        copy(y.at[at], out.at[at], 0).wait()
    if frames > 1:
        at = (slice(None), pl.ds(0, n_fq), slice(None), pl.ds(0, frames - 1))
        copy(y.at[at], out.at[at], 1).wait()
    copy(tail, out.at[:, pl.ds(0, n_fq), :, 0], 2).wait()


def shards(strengths, sample_cell, sample_frac):
    n_tm, n_fq = lax.axis_size("tm"), lax.axis_size("freq")
    parts, groups, channels, samples = strengths.shape
    span = n_tm // n_fq
    frames = span // PER_FRAME
    chunk = channels // n_tm
    rows = parts * chunk
    total = groups * n_tm * rows
    low = np.arange(FFT_LO)[:, None] * np.arange(FFT_HI)[None, :] * (2 * math.pi / FFTLEN)
    high = np.arange(FFT_HI)[:, None] * np.arange(FFT_HI)[None, :] % FFT_HI * (2 * math.pi / FFT_HI)
    hc, hs = np.cos(high), np.sin(high)
    full = np.block([[hc, -hs], [hs, hc]]).astype(np.float32) / math.sqrt(FFTLEN)
    vmem = pl.BlockSpec(memory_space=pltpu.VMEM)
    y_shape = (parts, n_fq * groups, chunk, frames, FFT_LO, FFT_HI)
    results = pl.pallas_call(
        functools.partial(main_kernel, n_tm, n_fq),
        out_shape=(
            pltpu.VMEM(y_shape, jnp.float32),
            pltpu.VMEM((n_fq, span, groups, SLABS, rows, LANES), jnp.bfloat16),
            pltpu.VMEM((FFT_LO, FFT_HI), jnp.float32),
            pltpu.VMEM((FFT_LO, FFT_HI), jnp.float32),
            pltpu.VMEM((2 * FFT_HI, 2 * FFT_HI), jnp.bfloat16),
        ),
        in_specs=[pl.BlockSpec(memory_space=pltpu.HBM)] * 6,
        out_specs=(vmem,) * 5,
        scratch_shapes=[
            pltpu.VMEM((parts, groups, channels, samples), jnp.bfloat16),
            pltpu.VMEM((samples // LANES, LANES), jnp.int32),
            pltpu.VMEM((samples // LANES, LANES), jnp.float32),
            pltpu.VMEM((samples, LANES), jnp.float32),
            pltpu.VMEM((samples, LANES), jnp.float32),
            pltpu.VMEM((samples, (SLABS + 1) * LANES), jnp.bfloat16),
            pltpu.VMEM((2, parts * HALF, total // parts), jnp.float32),
            pltpu.VMEM((2, parts * HALF, total // parts), jnp.float32),
            pltpu.VMEM((n_tm, groups, SLABS, rows, LANES), jnp.bfloat16),
            pltpu.VMEM((FFT_LO * chunk, 2 * FFT_HI), jnp.bfloat16),
            pltpu.SemaphoreType.DMA((5,)),
            pltpu.SemaphoreType.DMA((3,)),
            pltpu.SemaphoreType.DMA((2,)),
            pltpu.SemaphoreType.DMA((n_fq, frames, groups)),
            pltpu.SemaphoreType.DMA((2,)),
            pltpu.SemaphoreType.DMA((2,)),
            pltpu.SemaphoreType.REGULAR,
        ],
        compiler_params=pltpu.CompilerParams(
            collective_id=0, has_side_effects=True, vmem_limit_bytes=48 * 1024 * 1024
        ),
        name="grid_exchange_transform",
    )(
        strengths,
        sample_cell.reshape(samples // LANES, LANES),
        sample_frac.reshape(samples // LANES, LANES),
        jnp.asarray(np.cos(low), jnp.float32),
        jnp.asarray(np.sin(low), jnp.float32),
        jnp.asarray(full.astype(jnp.bfloat16)),
    )
    return pl.pallas_call(
        functools.partial(last_kernel, n_fq),
        out_shape=jax.ShapeDtypeStruct(y_shape, jnp.float32),
        in_specs=[vmem] * 5,
        out_specs=pl.BlockSpec(memory_space=pl.ANY),
        scratch_shapes=[
            pltpu.VMEM((parts, n_fq, chunk, FFT_LO, FFT_HI), jnp.float32),
            pltpu.VMEM((FFT_LO * chunk, 2 * FFT_HI), jnp.bfloat16),
            pltpu.SemaphoreType.DMA((3,)),
        ],
        compiler_params=pltpu.CompilerParams(vmem_limit_bytes=16 * 1024 * 1024),
        name="last_units_write",
    )(*results)


def solution(mesh):
    placed = (P(None, "freq", None, "tm"), P("tm"), P("tm"))
    return jax.shard_map(
        shards,
        mesh=mesh,
        in_specs=placed,
        out_specs=P(None, None, "tm", "freq", None, None),
        check_vma=False,
    )
```
